16 devices in a mesh: dp: 4 (over y, z, core), sp: 4 (over x).
Axes of the slice: x: 4, y: 2, z: 1, core: 2. Of those that a mesh axis runs over, the one named last changes fastest.
The devices are a block of a 4x4x8 slice.
Arguments:
- x: bfloat16 [16384, 2048], P(('dp', 'sp')), parts along dimension 0
- gain: bfloat16 [2048], replicated
- wq: bfloat16 [2048, 2048], P('sp')
- wk: bfloat16 [2048, 1024], P('sp')
- wv: bfloat16 [2048, 1024], P('sp')
- wo: bfloat16 [2048, 2048], P('sp')
Outputs:
- output: bfloat16 [16384, 2048], P(('dp', 'sp')), parts along dimension 0
There are 4 independent parts. The reference program is written for one: setup_inputs(seed, part) draws one part's arguments, and reference() takes and returns one part's arrays. A program takes and returns all parts, laid end to end along the dimension named above; an argument that names none is the same for every part.
All inputs are finite; a program needn't handle non-finite values.
Results may differ from the reference program's by a relative error of at most 0.012.
Values are sent between devices in bfloat16 or wider.
A program may use at most 768 MiB of HBM per device.

```python
import jax
import jax.numpy as jnp
from jax import lax

ROWS = 4096
D = 2048
HEADS = 16
KV_HEADS = 8
HEAD = 128
THETA = 10000


def setup_inputs(seed: int = 0, part: int = 0) -> dict:
    kx, kn, kq, kk, kv, ko = jax.random.split(jax.random.key(seed), 6)

    def weights(key, rows, columns):
        return jax.random.normal(key, (rows, columns), jnp.float32) * rows**-0.5

    drawn = {
        "x": jax.random.normal(jax.random.fold_in(kx, part), (ROWS, D), jnp.float32),
        "gain": 1 + 0.1 * jax.random.normal(kn, (D,), jnp.float32),
        "wq": 2 * weights(kq, D, HEADS * HEAD),
        "wk": 2 * weights(kk, D, KV_HEADS * HEAD),
        "wv": 4 * weights(kv, D, KV_HEADS * HEAD),
        "wo": weights(ko, HEADS * HEAD, D),
    }
    return {k: v.astype(jnp.bfloat16) for k, v in drawn.items()}


def normed(x, gain):
    wide = x.astype(jnp.float32)
    scale = lax.rsqrt(jnp.mean(wide * wide, -1, keepdims=True) + 1e-6)
    return (wide * scale * gain.astype(jnp.float32)).astype(jnp.bfloat16)


def turned(t, place, theta):
    half = t.shape[-1] // 2
    angle = place.astype(jnp.float32)[:, None] * theta ** (-jnp.arange(half, dtype=jnp.float32) / half)
    cos, sin = jnp.cos(angle)[:, None], jnp.sin(angle)[:, None]
    a, b = t[..., :half].astype(jnp.float32), t[..., half:].astype(jnp.float32)
    return jnp.concatenate([a * cos - b * sin, b * cos + a * sin], -1).astype(jnp.bfloat16)


def matmul(a, w):
    return jnp.dot(a, w, preferred_element_type=jnp.float32).astype(jnp.bfloat16)


def einsum(form, a, b):
    return jnp.einsum(form, a.astype(jnp.float32), b.astype(jnp.float32))


def attention(q, k, v):
    scores = einsum("tgsd,ugd->gstu", q, k) * q.shape[-1] ** -0.5
    token = jnp.arange(q.shape[0])
    scores = jnp.where(token[:, None] >= token, scores, -jnp.inf)
    weights = jax.nn.softmax(scores, -1).astype(jnp.bfloat16)
    return einsum("gstu,ugd->tgsd", weights, v).astype(jnp.bfloat16)


def reference(x, gain, wq, wk, wv, wo):
    a, place = normed(x, gain), jnp.arange(ROWS)
    q = turned(matmul(a, wq).reshape(ROWS, HEADS, HEAD), place, THETA).reshape(ROWS, KV_HEADS, -1, HEAD)
    k = turned(matmul(a, wk).reshape(ROWS, KV_HEADS, HEAD), place, THETA)
    v = matmul(a, wv).reshape(ROWS, KV_HEADS, HEAD)
    seen = attention(q, k, v).reshape(ROWS, HEADS * HEAD)
    return (x.astype(jnp.float32) + jnp.dot(seen, wo, preferred_element_type=jnp.float32)).astype(jnp.bfloat16)
```

```python
import functools

import jax
import jax.numpy as jnp
from jax import lax
from jax.experimental import pallas as pl
from jax.experimental.pallas import tpu as pltpu
from jax.sharding import PartitionSpec as P

HEAD = 128
THETA = 10000
NEG = -1e30
HIDDEN = 2 * NEG
LOG2E = 1.4426950408889634
MESH = pl.DeviceIdType.MESH
TILE = 256
ROWS = 512
KEYS = 512
STRIP = 256
AHEAD = 3
SHARED = dict(wk=False, wv=False, wq=False, wo=False)


def _dot(a, b, ca, cb):
    return lax.dot_general(a, b, (((ca,), (cb,)), ((), ())), preferred_element_type=jnp.float32)


class Gather:
    def __init__(self, at, shard, full, sems, ids, wide):
        self.shard, self.full, self.wide = shard, full, wide
        self.send, self.recv = sems[0].at[at], sems[1].at[at]
        self.me, self.left, self.right, self.far, self.core, self.near, self.c, self.p = ids
        self.rows = shard.shape[0]
        self.n = self.rows // (4 if wide else 2)

    def lane(self, p, c):
        return (p * 2 + c) * self.n if self.wide else c * self.n

    def piece(self, k, lane):
        n, q = self.n, self.n // 2
        block, off, size = ((self.left, 0, n), (self.right, 0, n), (self.far, 0, q), (self.far, q, q))[k]
        return self.full.at[pl.ds(pl.multiple_of(block * self.rows + lane + off, 16), size), :]

    def copy(self, src, dst, k, to):
        return pltpu.make_async_remote_copy(src, dst, self.send.at[k], self.recv.at[k], device_id=to, device_id_type=MESH)

    def go(self, src, dst, k, to):
        self.copy(src, dst, k, to).start()

    def arrived(self, k, lane, group):
        ref = self.piece(k, lane)
        self.copy(ref, ref, group * 4 + k, {"dp": self.core}).wait_recv()

    def begin(self):
        lane = self.lane(self.p, self.c)
        src = self.shard.at[pl.ds(pl.multiple_of(lane, 16), self.n), :]
        dst = self.full.at[pl.ds(pl.multiple_of(self.me * self.rows + lane, 16), self.n), :]
        self.go(src, dst, 0, {"sp": self.right})
        self.go(src, dst, 1, {"sp": self.left})

    def hand(self, k):
        ref = self.piece(k, self.lane(self.p, self.c))
        if self.wide:
            self.go(ref, ref, 4 + k, {"dp": self.near})
        self.go(ref, ref, 8 + k, {"dp": self.core})

    def relay(self):
        lane, q = self.lane(self.p, self.c), self.n // 2
        for k, block, off, to in ((0, self.left, 0, self.right), (1, self.right, q, self.left)):
            self.arrived(k, lane, 0)
            ref = self.full.at[pl.ds(pl.multiple_of(block * self.rows + lane + off, 16), q), :]
            self.go(ref, ref, 2 + k, {"sp": to})
            self.hand(k)

    def spread(self):
        for k in (2, 3):
            self.arrived(k, self.lane(self.p, self.c), 0)
            self.hand(k)
        if self.wide:
            for k in range(4):
                lane = self.lane(1 - self.p, self.c)
                self.arrived(k, lane, 1)
                ref = self.piece(k, lane)
                self.go(ref, ref, 12 + k, {"dp": self.core})

    def finish(self):
        for k in range(4):
            self.arrived(k, self.lane(self.p, 1 - self.c), 2)
        if self.wide:
            for k in range(4):
                self.arrived(k, self.lane(1 - self.p, 1 - self.c), 3)

    def drain(self):
        for k in range(16):
            if self.wide or k // 4 in (0, 2):
                ref = self.piece(k % 4, self.lane(self.p, self.c))
                self.copy(ref, ref, k, {"dp": self.core}).wait_send()


def kernel(ring, x_ref, gain_ref, freq_ref, wq_ref, wk_ref, wv_ref, wo_ref, seen_ref, wof_ref,
           a_s, wk_s, wv_s, wq_s, q_s, kv_s, cos_s, sin_s, top_s, mix_s, local, wsend, wrecv, ksend, krecv):
    me, group = lax.axis_index("sp"), lax.axis_index("dp")
    left, right, far = lax.rem(me + ring - 1, ring), lax.rem(me + 1, ring), lax.rem(me + 2, ring)
    c, p = lax.rem(group, 2), lax.rem(lax.div(group, 2), 2)
    core, near = group + 1 - 2 * c, group + 2 - 4 * p
    own, depth = x_ref.shape
    heads = kv_s.shape[1]
    wide = any(SHARED.values())

    barrier = pltpu.get_barrier_semaphore()
    peers = [{"sp": left}, {"sp": right}, {"dp": core}] + ([{"dp": near}] if wide else [])
    for peer in peers:
        pl.semaphore_signal(barrier, inc=1, device_id=peer, device_id_type=MESH)
    pl.semaphore_wait(barrier, len(peers))

    ids = me, left, right, far, core, near, c, p
    sems = wsend, wrecv
    gk = Gather(0, wk_ref, wk_s, sems, ids, SHARED["wk"])
    gv = Gather(1, wv_ref, wv_s, sems, ids, SHARED["wv"])
    gq = Gather(2, wq_ref, wq_s, sems, ids, SHARED["wq"])
    go = Gather(3, wo_ref, wof_ref, sems, ids, SHARED["wo"])
    gk.begin()
    gv.begin()

    def mine(full, shard):
        return full.at[pl.ds(pl.multiple_of(me * shard.shape[0], 16), shard.shape[0]), :]

    loads = [pltpu.make_async_copy(x_ref, a_s, local.at[0]), pltpu.make_async_copy(wk_ref, mine(wk_s, wk_ref), local.at[1]),
             pltpu.make_async_copy(wv_ref, mine(wv_s, wv_ref), local.at[2]), pltpu.make_async_copy(wq_ref, mine(wq_s, wq_ref), local.at[3]),
             pltpu.make_async_copy(wo_ref, mine(wof_ref, wo_ref), local.at[4])]
    for load in loads:
        load.start()

    loads[0].wait()
    gain = gain_ref[...].astype(jnp.float32)

    def norm(i, _):
        rows = pl.ds(pl.multiple_of(i * 64, 64), 64)
        wide = a_s[rows, :].astype(jnp.float32)
        scale = lax.rsqrt(jnp.mean(wide * wide, -1, keepdims=True) + 1e-6)
        a_s[rows, :] = (wide * scale * gain).astype(jnp.bfloat16)

    lax.fori_loop(0, own // 64, norm, None)

    def angles(i, _):
        rows = pl.ds(pl.multiple_of(i * 128, 128), 128)
        place = me * own + i * 128 + lax.broadcasted_iota(jnp.int32, (128, HEAD), 0)
        angle = place.astype(jnp.float32) * freq_ref[...]
        cos_s[rows, :] = jnp.cos(angle)
        sine = jnp.sin(angle)
        sin_s[rows, :] = jnp.where(lax.broadcasted_iota(jnp.int32, (128, HEAD), 1) < HEAD // 2, -sine, sine)

    lax.fori_loop(0, own // 128, angles, None)

    def turned(t, rows):
        wide = t.astype(jnp.float32)
        return (wide * cos_s[rows, :] + pltpu.roll(wide, HEAD // 2, 1) * sin_s[rows, :]).astype(jnp.bfloat16)

    def project(w_s, n, rows):
        cols = pl.ds(pl.multiple_of(n * TILE, TILE), TILE)
        return jnp.dot(a_s[rows, :], w_s[:, cols], preferred_element_type=jnp.float32).astype(jnp.bfloat16)

    def copy(j, part, h, kind, to):
        ref = kv_s.at[j, h, part]
        return pltpu.make_async_remote_copy(ref, ref, ksend.at[kind, part, h], krecv.at[j, part, h], device_id={"sp": to}, device_id_type=MESH)

    last = ring - 1

    def flows(h):
        sends = [(0, 0, 0, 0), (0, 0, 1, 0), (0, 0, 0, 1), (0, 0, 1, 1), (1, 1, 0, 0), (1, 1, 1, 0), (1, 1, 1, 1), (2, 2, 0, 0), (2, 2, 1, 0)]
        passed = [(last, 0, 0, 1), (last, 0, 1, 1), (2, 1, 0, 0), (0, 1, 1, 1)]
        return sends, passed

    def send(h):
        sends, _ = flows(h)
        for device in range(ring):
            todo = [f for f in sends if f[0] == device]
            if todo:
                @pl.when(me == device)
                def _():
                    for _, j, part, way in todo:
                        copy(j, part, h, way, left if way else right).start()

    def pass_on(h):
        _, passed = flows(h)
        for device in range(ring):
            todo = [f for f in passed if f[0] == device]
            if todo:
                @pl.when(me == device)
                def _():
                    for _, j, part, way in todo:
                        copy(j, part, h, 2, left if way else right).wait_recv()
                        copy(j, part, h, 2, left if way else right).start()

    def await_keys(h):
        _, passed = flows(h)
        for device in range(ring):
            done = [f[1:3] for f in passed if f[0] == device]
            todo = [(j, part) for j in range(device) for part in range(2) if (j, part) not in done]
            if todo:
                @pl.when(me == device)
                def _():
                    for j, part in todo:
                        copy(j, part, h, 2, right).wait_recv()

    def drain(h):
        sends, passed = flows(h)
        for device in range(ring):
            todo = [(f[1], f[2], f[3]) for f in sends if f[0] == device] + [(f[1], f[2], 2) for f in passed if f[0] == device]
            if todo:
                @pl.when(me == device)
                def _():
                    for j, part, kind in todo:
                        copy(j, part, h, kind, right).wait_send()

    gk.relay()
    gv.relay()
    gq.begin()
    gk.spread()
    gk.finish()
    loads[1].wait()

    tiles = own // ROWS

    def keys(i, _):
        n, m = lax.div(i, tiles), lax.rem(i, tiles)
        rows = pl.ds(pl.multiple_of(m * ROWS, ROWS), ROWS)
        t = project(wk_s, n, rows)
        for g in range(2):
            kv_s[me, 2 * n + g, 0, rows, :] = turned(t[:, g * HEAD : (g + 1) * HEAD], rows)

    lax.fori_loop(0, heads // 2 * tiles, keys, None)

    gv.spread()
    gv.finish()
    loads[2].wait()

    def values(i, _):
        n, m = lax.div(i, tiles), lax.rem(i, tiles)
        rows = pl.ds(pl.multiple_of(m * ROWS, ROWS), ROWS)
        t = project(wv_s, n, rows)
        for g in range(2):
            kv_s[me, 2 * n + g, 1, rows, :] = t[:, g * HEAD : (g + 1) * HEAD]

        @pl.when(i == tiles)
        def _():
            send(0)
            send(1)

    lax.fori_loop(0, heads // 2 * tiles, values, None)

    gq.relay()
    send(2)
    gq.spread()
    pass_on(0)
    gq.finish()
    loads[3].wait()

    e = HEAD**-0.5 * LOG2E
    cols = 2 * STRIP
    strips = own // STRIP

    def update(k, v, which, masked):
        scores = [_dot(k, q_s[s], 1, 1) for s in which]
        weights, keeps = [], []
        for s, t in zip(which, scores):
            if s == masked:
                t = jnp.where(lax.rem(lax.broadcasted_iota(jnp.int32, t.shape, 1), STRIP) >= lax.broadcasted_iota(jnp.int32, t.shape, 0), t, HIDDEN)
            old = top_s[s : s + 1, :]
            top = jnp.maximum(old, t.max(axis=0, keepdims=True))
            top_s[s : s + 1, :] = top
            weights.append(jnp.exp2((t - top) * e).astype(jnp.bfloat16))
            keeps.append(jnp.exp2((old - top) * e))
        lhs = jnp.concatenate([v.T, jnp.ones((8, v.shape[0]), jnp.bfloat16)], axis=0)
        for s, w, keep in zip(which, weights, keeps):
            mix_s[s] = mix_s[s] * keep + _dot(lhs, w, 1, 0)

    per = own // KEYS

    def head(h, _):
        @pl.when(h + AHEAD < heads)
        def _():
            send(h + AHEAD)

        @pl.when(h + 1 < heads)
        def _():
            pass_on(h + 1)

        for m in range(tiles):
            rows = pl.ds(m * ROWS, ROWS)
            t = project(wq_s, h, rows)
            for g in range(2):
                u = turned(t[:, g * HEAD : (g + 1) * HEAD], rows)
                for i in range(ROWS // STRIP):
                    q_s[m * (ROWS // STRIP) + i, g * STRIP : (g + 1) * STRIP, :] = u[i * STRIP : (i + 1) * STRIP, :]
        top_s[...] = jnp.full_like(top_s, NEG)
        mix_s[...] = jnp.zeros_like(mix_s)
        await_keys(h)

        def block(j, _):
            at = pl.ds(pl.multiple_of(lax.rem(j, per) * KEYS, KEYS), KEYS)
            ch = lax.div(j, per)
            update(kv_s[ch, h, 0, at, :], kv_s[ch, h, 1, at, :], range(strips), None)

        lax.fori_loop(0, me * per, block, None)
        for b in range(strips):
            at = pl.ds(b * STRIP, STRIP)
            update(kv_s[me, h, 0, at, :], kv_s[me, h, 1, at, :], range(b, strips), b)
        for s in range(strips):
            out = (mix_s[s, :HEAD, :] * (1 / mix_s[s, HEAD : HEAD + 1, :])).T.astype(jnp.bfloat16)
            for g in range(2):
                place = pl.ds(pl.multiple_of(h * 2 * HEAD + g * HEAD, HEAD), HEAD)
                seen_ref[s * STRIP : (s + 1) * STRIP, place] = out[g * STRIP : (g + 1) * STRIP, :]

        @pl.when(h == heads - 3)
        def _():
            go.begin()

    lax.fori_loop(0, heads, head, None)

    go.relay()
    go.spread()
    go.finish()
    loads[4].wait()
    for g in (gk, gv, gq, go):
        g.drain()
    lax.fori_loop(0, heads, lambda h, _: drain(h), None)


def solution(mesh):
    ring = mesh.shape["sp"]

    def step(x, gain, wq, wk, wv, wo):
        own, depth = x.shape
        heads = wk.shape[1] // HEAD
        half = HEAD // 2
        freq = THETA ** (-jnp.arange(half, dtype=jnp.float32) / half)
        freq = jnp.concatenate([freq, freq])[None]
        full = lambda w: pltpu.VMEM((w.shape[0] * ring, w.shape[1]), w.dtype)
        anywhere, vmem = pl.BlockSpec(memory_space=pl.ANY), pl.BlockSpec(memory_space=pltpu.VMEM)
        strips = own // STRIP
        seen, wof = pl.pallas_call(
            functools.partial(kernel, ring),
            out_shape=[jax.ShapeDtypeStruct((own, wq.shape[1]), x.dtype), jax.ShapeDtypeStruct((wo.shape[0] * ring, wo.shape[1]), wo.dtype)],
            in_specs=[anywhere, vmem, vmem, anywhere, anywhere, anywhere, anywhere],
            out_specs=[vmem, anywhere],
            scratch_shapes=[
                pltpu.VMEM((own, depth), jnp.bfloat16),
                full(wk),
                full(wv),
                full(wq),
                pltpu.VMEM((strips, 2 * STRIP, HEAD), jnp.bfloat16),
                pltpu.VMEM((ring, heads, 2, own, HEAD), jnp.bfloat16),
                pltpu.VMEM((own, HEAD), jnp.float32),
                pltpu.VMEM((own, HEAD), jnp.float32),
                pltpu.VMEM((strips, 2 * STRIP), jnp.float32),
                pltpu.VMEM((strips, HEAD + 8, 2 * STRIP), jnp.float32),
                pltpu.SemaphoreType.DMA((5,)),
                pltpu.SemaphoreType.DMA((4, 16)),
                pltpu.SemaphoreType.DMA((4, 16)),
                pltpu.SemaphoreType.DMA((3, 2, heads)),
                pltpu.SemaphoreType.DMA((ring, 2, heads)),
            ],
            compiler_params=pltpu.CompilerParams(collective_id=0, has_side_effects=True, vmem_limit_bytes=62 * 2**20),
        )(x, gain[None], freq, wq, wk, wv, wo)
        y = jnp.dot(seen, wof, preferred_element_type=jnp.float32)
        return (x.astype(jnp.float32) + y).astype(jnp.bfloat16)

    tokens, whole = P(("dp", "sp"), None), P("sp", None)
    return jax.shard_map(
        step,
        mesh=mesh,
        in_specs=(tokens, P(None), whole, whole, whole, whole),
        out_specs=tokens,
        check_vma=False,
    )
```

```python
import functools

import jax
import jax.numpy as jnp
from jax import lax
from jax.experimental import pallas as pl
from jax.experimental.pallas import tpu as pltpu
from jax.sharding import PartitionSpec as P

HEAD = 128
THETA = 10000
NEG = -1e30
HIDDEN = 2 * NEG
LOG2E = 1.4426950408889634
MESH = pl.DeviceIdType.MESH
TILE = 256
ROWS = 512
KEYS = 512
STRIP = 256
AHEAD = 4
NEAR = dict(wk=64, wv=64, wq=64, wo=128)
MOVED = 0


def _dot(a, b, ca, cb):
    return lax.dot_general(a, b, (((ca,), (cb,)), ((), ())), preferred_element_type=jnp.float32)


class Gather:
    def __init__(self, at, shard, full, sems, ids, y):
        self.shard, self.full, self.y = shard, full, y
        self.send, self.recv = sems[0].at[at], sems[1].at[at]
        self.me, self.left, self.right, self.far, self.core, self.near, self.c, self.p = ids
        self.rows = shard.shape[0]
        self.half = self.rows // 2
        self.n = self.half - y
        self.q = (self.n // 2 + 15) // 16 * 16

    def ring_lane(self, p, c):
        return c * self.half + p * self.y

    def near_lane(self, p, c):
        return c * self.half + p * (self.half - self.y)

    def at(self, b, off, size):
        block = (self.left, self.right, self.far)[b]
        return self.full.at[pl.ds(pl.multiple_of(block * self.rows + off, 16), size), :]

    def piece(self, k, p, c):
        if k < 4:
            off, size = ((0, self.n), (0, self.n), (0, self.q), (self.q, self.n - self.q))[k]
            return self.at(min(k, 2), self.ring_lane(p, c) + off, size)
        b, kind = (k - 4) % 3, (k - 4) // 3
        return self.at(b, self.ring_lane(p, c), self.n) if kind == 1 else self.at(b, self.near_lane(p, c), self.y)

    def copy(self, src, dst, k, to):
        return pltpu.make_async_remote_copy(src, dst, self.send.at[k], self.recv.at[k], device_id=to, device_id_type=MESH)

    def arrived(self, k, p, c):
        ref = self.piece(k, p, c)
        self.copy(ref, ref, k, {"dp": self.core}).wait_recv()

    def begin(self):
        lane = self.ring_lane(self.p, self.c)
        src = self.shard.at[pl.ds(pl.multiple_of(lane, 16), self.n), :]
        dst = self.full.at[pl.ds(pl.multiple_of(self.me * self.rows + lane, 16), self.n), :]
        self.copy(src, dst, 0, {"sp": self.right}).start()
        self.copy(src, dst, 1, {"sp": self.left}).start()

    def hand(self, b):
        if self.y:
            ref = self.piece(4 + b, self.p, self.c)
            self.copy(ref, ref, 4 + b, {"dp": self.near}).start()
        ref = self.piece(7 + b, self.p, self.c)
        self.copy(ref, ref, 7 + b, {"dp": self.core}).start()

    def relay(self):
        lane = self.ring_lane(self.p, self.c)
        for k, off, size, to in ((0, 0, self.q, self.right), (1, self.q, self.n - self.q, self.left)):
            self.arrived(k, self.p, self.c)
            ref = self.at(k, lane + off, size)
            self.copy(ref, ref, 2 + k, {"sp": to}).start()
            self.hand(k)

    def cross(self, b):
        if self.y:
            self.arrived(4 + b, 1 - self.p, self.c)
            ref = self.piece(10 + b, 1 - self.p, self.c)
            self.copy(ref, ref, 10 + b, {"dp": self.core}).start()

    def spread(self):
        for b in (0, 1):
            self.cross(b)
        for k in (2, 3):
            self.arrived(k, self.p, self.c)
        self.hand(2)
        self.cross(2)

    def finish(self):
        for b in range(3):
            self.arrived(7 + b, self.p, 1 - self.c)
            if self.y:
                self.arrived(10 + b, 1 - self.p, 1 - self.c)

    def drain(self):
        for k in range(13):
            if self.y or k not in (4, 5, 6, 10, 11, 12):
                ref = self.piece(k, self.p, self.c)
                self.copy(ref, ref, k, {"dp": self.core}).wait_send()


def kernel(ring, x_ref, gain_ref, freq_ref, wq_ref, wk_ref, wv_ref, wo_ref, seen_ref, wof_ref,
           a_s, wk_s, wv_s, wq_s, q_s, moved_s, kv_s, out_s, seen_s, cos_s, sin_s, top_s, mix_s,
           local, store, wsend, wrecv, ksend, krecv, qsend, qrecv, osend, orecv):
    me, group = lax.axis_index("sp"), lax.axis_index("dp")
    left, right, far = lax.rem(me + ring - 1, ring), lax.rem(me + 1, ring), lax.rem(me + 2, ring)
    c, p = lax.rem(group, 2), lax.rem(lax.div(group, 2), 2)
    core, near = group + 1 - 2 * c, group + 2 - 4 * p
    own, depth = x_ref.shape
    heads = kv_s.shape[1]
    wide = any(NEAR.values())

    barrier = pltpu.get_barrier_semaphore()
    peers = [{"sp": left}, {"sp": right}, {"dp": core}] + ([{"dp": near}] if wide else [])
    for peer in peers:
        pl.semaphore_signal(barrier, inc=1, device_id=peer, device_id_type=MESH)
    pl.semaphore_wait(barrier, len(peers))

    ids = me, left, right, far, core, near, c, p
    sems = wsend, wrecv
    gk = Gather(0, wk_ref, wk_s, sems, ids, NEAR["wk"])
    gv = Gather(1, wv_ref, wv_s, sems, ids, NEAR["wv"])
    gq = Gather(2, wq_ref, wq_s, sems, ids, NEAR["wq"])
    go = Gather(3, wo_ref, wof_ref, sems, ids, NEAR["wo"])
    gk.begin()
    gv.begin()

    def mine(full, shard):
        return full.at[pl.ds(pl.multiple_of(me * shard.shape[0], 16), shard.shape[0]), :]

    loads = [pltpu.make_async_copy(x_ref, a_s, local.at[0]), pltpu.make_async_copy(wk_ref, mine(wk_s, wk_ref), local.at[1]),
             pltpu.make_async_copy(wv_ref, mine(wv_s, wv_ref), local.at[2]), pltpu.make_async_copy(wq_ref, mine(wq_s, wq_ref), local.at[3]),
             pltpu.make_async_copy(wo_ref, mine(wof_ref, wo_ref), local.at[4])]
    for load in loads:
        load.start()

    loads[0].wait()
    gain = gain_ref[...].astype(jnp.float32)

    def norm(i, _):
        rows = pl.ds(pl.multiple_of(i * 64, 64), 64)
        wide = a_s[rows, :].astype(jnp.float32)
        scale = lax.rsqrt(jnp.mean(wide * wide, -1, keepdims=True) + 1e-6)
        a_s[rows, :] = (wide * scale * gain).astype(jnp.bfloat16)

    lax.fori_loop(0, own // 64, norm, None)

    def angles(i, _):
        rows = pl.ds(pl.multiple_of(i * 128, 128), 128)
        place = me * own + i * 128 + lax.broadcasted_iota(jnp.int32, (128, HEAD), 0)
        angle = place.astype(jnp.float32) * freq_ref[...]
        cos_s[rows, :] = jnp.cos(angle)
        sine = jnp.sin(angle)
        sin_s[rows, :] = jnp.where(lax.broadcasted_iota(jnp.int32, (128, HEAD), 1) < HEAD // 2, -sine, sine)

    lax.fori_loop(0, own // 128, angles, None)

    def turned(t, rows):
        wide = t.astype(jnp.float32)
        return (wide * cos_s[rows, :] + pltpu.roll(wide, HEAD // 2, 1) * sin_s[rows, :]).astype(jnp.bfloat16)

    def project(w_s, n, rows):
        cols = pl.ds(pl.multiple_of(n * TILE, TILE), TILE)
        return jnp.dot(a_s[rows, :], w_s[:, cols], preferred_element_type=jnp.float32).astype(jnp.bfloat16)

    def copy(j, part, h, kind, to):
        ref = kv_s.at[j, h, part]
        return pltpu.make_async_remote_copy(ref, ref, ksend.at[kind, part, h], krecv.at[j, part, h], device_id={"sp": to}, device_id_type=MESH)

    def moved(h):
        return lax.rem(jnp.int32(h), 2) == MOVED

    last = ring - 1
    SENDS = [(0, 0, 0), (0, 0, 1), (1, 1, 0), (2, 2, 0)], [(0, 0, 0), (1, 1, 1), (2, 2, 1), (3, 3, 0)]
    PASSED = [(last, 0, 1), (2, 1, 0)], [(1, 2, 1)]
    NEEDED = [(1, 0), (2, 0), (2, 1), (3, 0), (3, 1), (3, 2)], [(0, 1), (0, 2), (0, 3), (1, 0), (1, 2)]

    def each(table, h, act):
        for kind_of_head in (0, 1):
            for device in range(ring):
                rows = [f for f in table[kind_of_head] if f[0] == device]
                if rows:
                    @pl.when((me == device) & (moved(h) == bool(kind_of_head)))
                    def _():
                        for f in rows:
                            for part in range(2):
                                act(f[1], part, f[2] if len(f) > 2 else 0)

    def send(h):
        each(SENDS, h, lambda j, part, way: copy(j, part, h, way, left if way else right).start())

    def pass_on(h):
        def act(j, part, way):
            copy(j, part, h, 2, left if way else right).wait_recv()
            copy(j, part, h, 2, left if way else right).start()

        each(PASSED, h, act)

    def await_keys(h):
        rest = tuple([f for f in NEEDED[i] if f not in [g[:2] for g in PASSED[i]]] for i in (0, 1))
        each(rest, h, lambda j, part, way: copy(j, part, h, 2, right).wait_recv())

    def drain(h):
        each(SENDS, h, lambda j, part, way: copy(j, part, h, way, right).wait_send())
        each(PASSED, h, lambda j, part, way: copy(j, part, h, 2, right).wait_send())

    early, partner = me < ring // 2, ring - 1 - me

    def to_partner(h, ref, dst, send_sem, recv_sem):
        slot = lax.div(jnp.int32(h), 2)
        return pltpu.make_async_remote_copy(ref, dst, send_sem.at[slot], recv_sem.at[slot], device_id={"sp": partner}, device_id_type=MESH)

    def query(h):
        ref = moved_s.at[lax.div(jnp.int32(h), 2)]
        return to_partner(h, ref, ref, qsend, qrecv)

    def panel(ref, h):
        return ref.at[:, pl.ds(pl.multiple_of(h * 2 * HEAD, 2 * HEAD), 2 * HEAD)]

    def result(h):
        return to_partner(h, out_s.at[lax.div(jnp.int32(h), 2)], panel(seen_s, h), osend, orecv)

    def keep(h):
        return pltpu.make_async_copy(panel(seen_s, h), panel(seen_ref, h), store.at[h])

    def send_query(h):
        @pl.when(moved(h) & jnp.logical_not(early))
        def _():
            query(h).start()

    gk.relay()
    gv.relay()
    gq.begin()
    gk.spread()
    gk.finish()
    loads[1].wait()

    tiles = own // ROWS

    def keys(i, _):
        n, m = lax.div(i, tiles), lax.rem(i, tiles)
        rows = pl.ds(pl.multiple_of(m * ROWS, ROWS), ROWS)
        t = project(wk_s, n, rows)
        for g in range(2):
            kv_s[me, 2 * n + g, 0, rows, :] = turned(t[:, g * HEAD : (g + 1) * HEAD], rows)

    lax.fori_loop(0, heads // 2 * tiles, keys, None)

    gv.spread()
    gv.finish()
    loads[2].wait()

    def values(i, _):
        n, m = lax.div(i, tiles), lax.rem(i, tiles)
        rows = pl.ds(pl.multiple_of(m * ROWS, ROWS), ROWS)
        t = project(wv_s, n, rows)
        for g in range(2):
            kv_s[me, 2 * n + g, 1, rows, :] = t[:, g * HEAD : (g + 1) * HEAD]

    lax.fori_loop(0, heads // 2 * tiles, values, None)

    gq.relay()
    for h in range(AHEAD):
        send(h)
    gq.spread()
    gq.finish()
    loads[3].wait()

    strips = own // STRIP

    def project_query(h, ref):
        for m in range(tiles):
            rows = pl.ds(m * ROWS, ROWS)
            t = project(wq_s, h, rows)
            for g in range(2):
                u = turned(t[:, g * HEAD : (g + 1) * HEAD], rows)
                for i in range(ROWS // STRIP):
                    ref[m * (ROWS // STRIP) + i, g * STRIP : (g + 1) * STRIP, :] = u[i * STRIP : (i + 1) * STRIP, :]

    @pl.when(jnp.logical_not(early))
    def _():
        def ask(i, _):
            project_query(2 * i + MOVED, moved_s.at[i])

            @pl.when(2 * i + MOVED < AHEAD)
            def _():
                query(2 * i + MOVED).start()

        lax.fori_loop(0, heads // 2, ask, None)

    pass_on(0)

    e = HEAD**-0.5 * LOG2E

    def update(q, k, v, which, masked):
        scores = [_dot(k, q[s], 1, 1) for s in which]
        weights, keeps = [], []
        for s, t in zip(which, scores):
            if s == masked:
                t = jnp.where(lax.rem(lax.broadcasted_iota(jnp.int32, t.shape, 1), STRIP) >= lax.broadcasted_iota(jnp.int32, t.shape, 0), t, HIDDEN)
            old = top_s[s : s + 1, :]
            top = jnp.maximum(old, t.max(axis=0, keepdims=True))
            top_s[s : s + 1, :] = top
            weights.append(jnp.exp2((t - top) * e).astype(jnp.bfloat16))
            keeps.append(jnp.exp2((old - top) * e))
        lhs = jnp.concatenate([v.T, jnp.ones((8, v.shape[0]), jnp.bfloat16)], axis=0)
        for s, w, keep in zip(which, weights, keeps):
            mix_s[s] = mix_s[s] * keep + _dot(lhs, w, 1, 0)

    per = own // KEYS

    def attend(h, q, chunk, put):
        top_s[...] = jnp.full_like(top_s, NEG)
        mix_s[...] = jnp.zeros_like(mix_s)

        def block(j, _):
            at = pl.ds(pl.multiple_of(lax.rem(j, per) * KEYS, KEYS), KEYS)
            ch = lax.div(j, per)
            update(q, kv_s[ch, h, 0, at, :], kv_s[ch, h, 1, at, :], range(strips), None)

        lax.fori_loop(0, chunk * per, block, None)
        for b in range(strips):
            at = pl.ds(b * STRIP, STRIP)
            update(q, kv_s[chunk, h, 0, at, :], kv_s[chunk, h, 1, at, :], range(b, strips), b)
        for s in range(strips):
            out = (mix_s[s, :HEAD, :] * (1 / mix_s[s, HEAD : HEAD + 1, :])).T.astype(jnp.bfloat16)
            for g in range(2):
                put(s, g, out[g * STRIP : (g + 1) * STRIP, :])

    def head(h, _):
        @pl.when(h + AHEAD < heads)
        def _():
            send(h + AHEAD)
            send_query(h + AHEAD)

        @pl.when(h + 1 < heads)
        def _():
            pass_on(h + 1)

        here = early | jnp.logical_not(moved(h))

        @pl.when(here)
        def _():
            project_query(h, q_s)

        await_keys(h)

        @pl.when(moved(h) & early)
        def _():
            query(h).wait_recv()
            slot = lax.div(h, 2)

            def put(s, g, out):
                out_s[slot, s * STRIP : (s + 1) * STRIP, g * HEAD : (g + 1) * HEAD] = out

            attend(h, moved_s.at[slot], partner, put)
            result(h).start()

        @pl.when(here)
        def _():
            def put(s, g, out):
                place = pl.ds(pl.multiple_of(h * 2 * HEAD + g * HEAD, HEAD), HEAD)
                seen_s[s * STRIP : (s + 1) * STRIP, place] = out

            attend(h, q_s, me, put)
            keep(h).start()

        @pl.when(h == 1)
        def _():
            go.begin()

        @pl.when(h == 3)
        def _():
            go.relay()

        @pl.when(h == 5)
        def _():
            go.spread()

    lax.fori_loop(0, heads, head, None)

    def collect(h, _):
        @pl.when(moved(h) & jnp.logical_not(early))
        def _():
            result(h).wait_recv()
            keep(h).start()
            query(h).wait_send()

        @pl.when(moved(h) & early)
        def _():
            result(h).wait_send()

    lax.fori_loop(0, heads, collect, None)
    go.finish()
    loads[4].wait()
    for g in (gk, gv, gq, go):
        g.drain()

    def end(h, _):
        drain(h)
        keep(h).wait()

    lax.fori_loop(0, heads, end, None)


def solution(mesh):
    ring = mesh.shape["sp"]

    def step(x, gain, wq, wk, wv, wo):
        own, depth = x.shape
        heads = wk.shape[1] // HEAD
        half = HEAD // 2
        freq = THETA ** (-jnp.arange(half, dtype=jnp.float32) / half)
        freq = jnp.concatenate([freq, freq])[None]
        full = lambda w: pltpu.VMEM((w.shape[0] * ring, w.shape[1]), w.dtype)
        anywhere, vmem = pl.BlockSpec(memory_space=pl.ANY), pl.BlockSpec(memory_space=pltpu.VMEM)
        strips = own // STRIP
        seen, wof = pl.pallas_call(
            functools.partial(kernel, ring),
            out_shape=[jax.ShapeDtypeStruct((own, wq.shape[1]), x.dtype), jax.ShapeDtypeStruct((wo.shape[0] * ring, wo.shape[1]), wo.dtype)],
            in_specs=[anywhere, vmem, vmem, anywhere, anywhere, anywhere, anywhere],
            out_specs=[anywhere, anywhere],
            scratch_shapes=[
                pltpu.VMEM((own, depth), jnp.bfloat16),
                full(wk),
                full(wv),
                full(wq),
                pltpu.VMEM((strips, 2 * STRIP, HEAD), jnp.bfloat16),
                pltpu.VMEM((heads // 2, strips, 2 * STRIP, HEAD), jnp.bfloat16),
                pltpu.VMEM((ring, heads, 2, own, HEAD), jnp.bfloat16),
                pltpu.VMEM((heads // 2, own, 2 * HEAD), jnp.bfloat16),
                pltpu.VMEM((own, wq.shape[1]), jnp.bfloat16),
                pltpu.VMEM((own, HEAD), jnp.float32),
                pltpu.VMEM((own, HEAD), jnp.float32),
                pltpu.VMEM((strips, 2 * STRIP), jnp.float32),
                pltpu.VMEM((strips, HEAD + 8, 2 * STRIP), jnp.float32),
                pltpu.SemaphoreType.DMA((5,)),
                pltpu.SemaphoreType.DMA((heads,)),
                pltpu.SemaphoreType.DMA((4, 13)),
                pltpu.SemaphoreType.DMA((4, 13)),
                pltpu.SemaphoreType.DMA((3, 2, heads)),
                pltpu.SemaphoreType.DMA((ring, 2, heads)),
                *[pltpu.SemaphoreType.DMA((heads // 2,))] * 4,
            ],
            compiler_params=pltpu.CompilerParams(collective_id=0, has_side_effects=True, vmem_limit_bytes=62 * 2**20),
        )(x, gain[None], freq, wq, wk, wv, wo)
        y = jnp.dot(seen, wof, preferred_element_type=jnp.float32)
        return (x.astype(jnp.float32) + y).astype(jnp.bfloat16)

    tokens, whole = P(("dp", "sp"), None), P("sp", None)
    return jax.shard_map(
        step,
        mesh=mesh,
        in_specs=(tokens, P(None), whole, whole, whole, whole),
        out_specs=tokens,
        check_vma=False,
    )
```

```python
import functools

import jax
import jax.numpy as jnp
from jax import lax
from jax.experimental import pallas as pl
from jax.experimental.pallas import tpu as pltpu
from jax.sharding import PartitionSpec as P

HEAD = 128
THETA = 10000
NEG = -1e30
HIDDEN = 2 * NEG
LOG2E = 1.4426950408889634
MESH = pl.DeviceIdType.MESH
TILE = 256
ROWS = 512
KEYS = 512
STRIP = 256
NEAR = dict(wk=64, wv=64, wq=128, wo=128)
STAY, MOVED = 1, 0


def _dot(a, b, ca, cb):
    return lax.dot_general(a, b, (((ca,), (cb,)), ((), ())), preferred_element_type=jnp.float32)


class Gather:
    def __init__(self, at, shard, full, sems, ids, y, column=0, columns=None):
        self.shard, self.full, self.y = shard, full, y
        self.columns = pl.ds(column, columns or shard.shape[1])
        self.send, self.recv = sems[0].at[at], sems[1].at[at]
        self.me, self.left, self.right, self.far, self.core, self.near, self.c, self.p = ids
        self.rows = shard.shape[0]
        self.half = self.rows // 2
        self.n = self.half - y
        self.q = (self.n // 2 + 15) // 16 * 16

    def ring_lane(self, p, c):
        return c * self.half + p * self.y

    def near_lane(self, p, c):
        return c * self.half + p * (self.half - self.y)

    def at(self, b, off, size):
        block = (self.left, self.right, self.far)[b]
        return self.full.at[pl.ds(pl.multiple_of(block * self.rows + off, 16), size), self.columns]

    def piece(self, k, p, c):
        if k < 4:
            off, size = ((0, self.n), (0, self.n), (0, self.q), (self.q, self.n - self.q))[k]
            return self.at(min(k, 2), self.ring_lane(p, c) + off, size)
        b, kind = (k - 4) % 3, (k - 4) // 3
        return self.at(b, self.ring_lane(p, c), self.n) if kind == 1 else self.at(b, self.near_lane(p, c), self.y)

    def copy(self, src, dst, k, to):
        return pltpu.make_async_remote_copy(src, dst, self.send.at[k], self.recv.at[k], device_id=to, device_id_type=MESH)

    def arrived(self, k, p, c):
        ref = self.piece(k, p, c)
        self.copy(ref, ref, k, {"dp": self.core}).wait_recv()

    def begin(self):
        lane = self.ring_lane(self.p, self.c)
        src = self.shard.at[pl.ds(pl.multiple_of(lane, 16), self.n), self.columns]
        dst = self.full.at[pl.ds(pl.multiple_of(self.me * self.rows + lane, 16), self.n), self.columns]
        self.copy(src, dst, 0, {"sp": self.right}).start()
        self.copy(src, dst, 1, {"sp": self.left}).start()

    def hand(self, b):
        if self.y:
            ref = self.piece(4 + b, self.p, self.c)
            self.copy(ref, ref, 4 + b, {"dp": self.near}).start()
        ref = self.piece(7 + b, self.p, self.c)
        self.copy(ref, ref, 7 + b, {"dp": self.core}).start()

    def relay(self):
        lane = self.ring_lane(self.p, self.c)
        for k, off, size, to in ((0, 0, self.q, self.right), (1, self.q, self.n - self.q, self.left)):
            self.arrived(k, self.p, self.c)
            ref = self.at(k, lane + off, size)
            self.copy(ref, ref, 2 + k, {"sp": to}).start()
            self.hand(k)

    def last(self):
        for k in (2, 3):
            self.arrived(k, self.p, self.c)
        self.hand(2)

    def cross(self):
        for b in range(3 if self.y else 0):
            self.arrived(4 + b, 1 - self.p, self.c)
            ref = self.piece(10 + b, 1 - self.p, self.c)
            self.copy(ref, ref, 10 + b, {"dp": self.core}).start()

    def finish(self):
        for b in range(3):
            self.arrived(7 + b, self.p, 1 - self.c)
            if self.y:
                self.arrived(10 + b, 1 - self.p, 1 - self.c)

    def drain(self):
        for k in range(13):
            if self.y or k not in (4, 5, 6, 10, 11, 12):
                ref = self.piece(k, self.p, self.c)
                self.copy(ref, ref, k, {"dp": self.core}).wait_send()


def kernel(ring, x_ref, gain_ref, freq_ref, wq_ref, wk_ref, wv_ref, wo_ref, seen_ref, wof_ref,
           a_s, wk_s, wv_s, wq_s, q_s, moved_s, kv_s, out_s, seen_s, cos_s, sin_s, top_s, mix_s,
           local, store, wsend, wrecv, ksend, krecv, qsend, qrecv, osend, orecv):
    me, group = lax.axis_index("sp"), lax.axis_index("dp")
    left, right, far = lax.rem(me + ring - 1, ring), lax.rem(me + 1, ring), lax.rem(me + 2, ring)
    c, p = lax.rem(group, 2), lax.rem(lax.div(group, 2), 2)
    core, near = group + 1 - 2 * c, group + 2 - 4 * p
    own, depth = x_ref.shape
    heads = kv_s.shape[1]
    wide = any(NEAR.values())

    barrier = pltpu.get_barrier_semaphore()
    peers = [{"sp": left}, {"sp": right}, {"dp": core}] + ([{"dp": near}] if wide else [])
    for peer in peers:
        pl.semaphore_signal(barrier, inc=1, device_id=peer, device_id_type=MESH)
    pl.semaphore_wait(barrier, len(peers))

    ids = me, left, right, far, core, near, c, p
    sems = wsend, wrecv
    gk = Gather(0, wk_ref, wk_s, sems, ids, NEAR["wk"])
    gv = Gather(1, wv_ref, wv_s, sems, ids, NEAR["wv"])
    pairs = heads // 2
    wide_q = wq_ref.shape[1] // pairs
    go = Gather(2, wo_ref, wof_ref, sems, ids, NEAR["wo"])
    gq = [Gather(3 + i, wq_ref, wq_s, sems, ids, NEAR["wq"], i * wide_q, wide_q) for i in range(pairs)]
    gk.begin()
    gv.begin()

    def mine(full, shard):
        return full.at[pl.ds(pl.multiple_of(me * shard.shape[0], 16), shard.shape[0]), :]

    loads = [pltpu.make_async_copy(x_ref, a_s, local.at[0]), pltpu.make_async_copy(wk_ref, mine(wk_s, wk_ref), local.at[1]),
             pltpu.make_async_copy(wv_ref, mine(wv_s, wv_ref), local.at[2]), pltpu.make_async_copy(wq_ref, mine(wq_s, wq_ref), local.at[3]),
             pltpu.make_async_copy(wo_ref, mine(wof_ref, wo_ref), local.at[4])]
    for load in loads:
        load.start()

    loads[0].wait()
    gain = gain_ref[...].astype(jnp.float32)

    def norm(i, _):
        rows = pl.ds(pl.multiple_of(i * 64, 64), 64)
        wide = a_s[rows, :].astype(jnp.float32)
        scale = lax.rsqrt(jnp.mean(wide * wide, -1, keepdims=True) + 1e-6)
        a_s[rows, :] = (wide * scale * gain).astype(jnp.bfloat16)

    lax.fori_loop(0, own // 64, norm, None)

    def angles(i, _):
        rows = pl.ds(pl.multiple_of(i * 128, 128), 128)
        place = me * own + i * 128 + lax.broadcasted_iota(jnp.int32, (128, HEAD), 0)
        angle = place.astype(jnp.float32) * freq_ref[...]
        cos_s[rows, :] = jnp.cos(angle)
        sine = jnp.sin(angle)
        sin_s[rows, :] = jnp.where(lax.broadcasted_iota(jnp.int32, (128, HEAD), 1) < HEAD // 2, -sine, sine)

    lax.fori_loop(0, own // 128, angles, None)

    def turned(t, rows):
        wide = t.astype(jnp.float32)
        return (wide * cos_s[rows, :] + pltpu.roll(wide, HEAD // 2, 1) * sin_s[rows, :]).astype(jnp.bfloat16)

    def project(w_s, n, rows):
        cols = pl.ds(pl.multiple_of(n * TILE, TILE), TILE)
        return jnp.dot(a_s[rows, :], w_s[:, cols], preferred_element_type=jnp.float32).astype(jnp.bfloat16)

    def copy(j, part, h, kind, to):
        ref = kv_s.at[j, h, part]
        return pltpu.make_async_remote_copy(ref, ref, ksend.at[kind, part, h], krecv.at[j, part, h], device_id={"sp": to}, device_id_type=MESH)

    last = ring - 1
    SENDS = [(0, 0, 0), (1, 1, 1), (2, 2, 1), (3, 3, 0)], [(0, 0, 0), (0, 0, 1), (1, 1, 0), (2, 2, 0)]
    PASSED = [(1, 2, 1)], [(last, 0, 1), (2, 1, 0)]
    NEEDED = [(0, 1), (0, 2), (0, 3), (1, 0), (1, 2)], [(1, 0), (2, 0), (2, 1), (3, 0), (3, 1), (3, 2)]

    def each(rows, act):
        for device in range(ring):
            mine = [f for f in rows if f[0] == device]
            if mine:
                @pl.when(me == device)
                def _():
                    for f in mine:
                        for part in range(2):
                            act(f[1], part, f[2] if len(f) > 2 else 0)

    def send(h, sort):
        each(SENDS[sort], lambda j, part, way: copy(j, part, h, way, left if way else right).start())

    def pass_on(h, sort):
        def act(j, part, way):
            copy(j, part, h, 2, left if way else right).wait_recv()
            copy(j, part, h, 2, left if way else right).start()

        each(PASSED[sort], act)

    def await_keys(h, sort):
        rest = [f for f in NEEDED[sort] if f not in [g[:2] for g in PASSED[sort]]]
        each(rest, lambda j, part, way: copy(j, part, h, 2, right).wait_recv())

    def drain(h, sort):
        each(SENDS[sort], lambda j, part, way: copy(j, part, h, way, right).wait_send())
        each(PASSED[sort], lambda j, part, way: copy(j, part, h, 2, right).wait_send())

    early, partner = me < ring // 2, ring - 1 - me

    def to_partner(i, ref, dst, send_sem, recv_sem):
        return pltpu.make_async_remote_copy(ref, dst, send_sem.at[i], recv_sem.at[i], device_id={"sp": partner}, device_id_type=MESH)

    def query(i):
        return to_partner(i, moved_s.at[i], moved_s.at[i], qsend, qrecv)

    def panel(ref, h):
        return ref.at[:, pl.ds(pl.multiple_of(h * 2 * HEAD, 2 * HEAD), 2 * HEAD)]

    def result(i):
        return to_partner(i, out_s.at[i], panel(seen_s, 2 * i + MOVED), osend, orecv)

    def keep(h):
        return pltpu.make_async_copy(panel(seen_s, h), panel(seen_ref, h), store.at[h])

    gk.relay()
    gv.relay()
    for g in gq:
        g.begin()
    gk.last()
    gk.cross()
    gv.last()
    gk.finish()
    loads[1].wait()

    tiles = own // ROWS

    def keys(i, _):
        n, m = lax.div(i, tiles), lax.rem(i, tiles)
        rows = pl.ds(pl.multiple_of(m * ROWS, ROWS), ROWS)
        t = project(wk_s, n, rows)
        for g in range(2):
            kv_s[me, 2 * n + g, 0, rows, :] = turned(t[:, g * HEAD : (g + 1) * HEAD], rows)

    lax.fori_loop(0, heads // 2 * tiles, keys, None)

    gv.cross()
    gq[0].relay()
    gv.finish()
    loads[2].wait()

    def values(i, _):
        n, m = lax.div(i, tiles), lax.rem(i, tiles)
        rows = pl.ds(pl.multiple_of(m * ROWS, ROWS), ROWS)
        t = project(wv_s, n, rows)
        for g in range(2):
            kv_s[me, 2 * n + g, 1, rows, :] = t[:, g * HEAD : (g + 1) * HEAD]

    lax.fori_loop(0, heads // 2 * tiles, values, None)

    gq[0].last()
    for g in gq[1:]:
        g.relay()
    send(MOVED, MOVED)
    send(STAY, STAY)
    loads[3].wait()
    gq[0].cross()
    gq[0].finish()

    strips = own // STRIP

    def project_query(h, ref):
        for m in range(tiles):
            rows = pl.ds(m * ROWS, ROWS)
            t = project(wq_s, h, rows)
            for g in range(2):
                u = turned(t[:, g * HEAD : (g + 1) * HEAD], rows)
                for i in range(ROWS // STRIP):
                    ref[m * (ROWS // STRIP) + i, g * STRIP : (g + 1) * STRIP, :] = u[i * STRIP : (i + 1) * STRIP, :]

    def ask(i):
        @pl.when(jnp.logical_not(early))
        def _():
            project_query(2 * i + MOVED, moved_s.at[i])
            query(i).start()

    ask(0)
    for g in gq[1:]:
        g.last()
    pass_on(MOVED, MOVED)

    e = HEAD**-0.5 * LOG2E

    def update(q, k, v, which, masked):
        scores = [_dot(k, q[s], 1, 1) for s in which]
        weights, keeps = [], []
        for s, t in zip(which, scores):
            if s == masked:
                t = jnp.where(lax.rem(lax.broadcasted_iota(jnp.int32, t.shape, 1), STRIP) >= lax.broadcasted_iota(jnp.int32, t.shape, 0), t, HIDDEN)
            old = top_s[s : s + 1, :]
            top = jnp.maximum(old, t.max(axis=0, keepdims=True))
            top_s[s : s + 1, :] = top
            weights.append(jnp.exp2((t - top) * e).astype(jnp.bfloat16))
            keeps.append(jnp.exp2((old - top) * e))
        lhs = jnp.concatenate([v.T, jnp.ones((8, v.shape[0]), jnp.bfloat16)], axis=0)
        for s, w, keep in zip(which, weights, keeps):
            mix_s[s] = mix_s[s] * keep + _dot(lhs, w, 1, 0)

    per = own // KEYS

    def attend(h, q, chunk, put):
        top_s[...] = jnp.full_like(top_s, NEG)
        mix_s[...] = jnp.zeros_like(mix_s)

        def block(j, _):
            at = pl.ds(pl.multiple_of(lax.rem(j, per) * KEYS, KEYS), KEYS)
            ch = lax.div(j, per)
            update(q, kv_s[ch, h, 0, at, :], kv_s[ch, h, 1, at, :], range(strips), None)

        lax.fori_loop(0, chunk * per, block, None)
        for b in range(strips):
            at = pl.ds(b * STRIP, STRIP)
            update(q, kv_s[chunk, h, 0, at, :], kv_s[chunk, h, 1, at, :], range(b, strips), b)
        for s in range(strips):
            out = (mix_s[s, :HEAD, :] * (1 / mix_s[s, HEAD : HEAD + 1, :])).T.astype(jnp.bfloat16)
            for g in range(2):
                put(s, g, out[g * STRIP : (g + 1) * STRIP, :])

    def put_own(h):
        def put(s, g, out):
            place = pl.ds(pl.multiple_of(h * 2 * HEAD + g * HEAD, HEAD), HEAD)
            seen_s[s * STRIP : (s + 1) * STRIP, place] = out

        return put

    def pair(i, _):
        more = i + 1 < pairs

        @pl.when(more)
        def _():
            send(2 * i + 2 + MOVED, MOVED)
            send(2 * i + 2 + STAY, STAY)

        @pl.when(i == 0)
        def _():
            go.begin()

        h = 2 * i + MOVED

        @pl.when(early)
        def _():
            project_query(h, q_s)

        await_keys(h, MOVED)

        @pl.when(early)
        def _():
            query(i).wait_recv()

            def put(s, g, out):
                out_s[i, s * STRIP : (s + 1) * STRIP, g * HEAD : (g + 1) * HEAD] = out

            attend(h, moved_s.at[i], partner, put)
            result(i).start()
            attend(h, q_s, me, put_own(h))
            keep(h).start()

        h = 2 * i + STAY
        pass_on(h, STAY)

        for n in range(1, pairs):
            @pl.when(i + 1 == n)
            def _():
                gq[n].cross()
                gq[n].finish()

        @pl.when(more)
        def _():
            ask(i + 1)
            pass_on(2 * i + 2 + MOVED, MOVED)

        for n, act in ((1, go.relay), (2, go.last), (3, go.cross)):
            @pl.when(i == n)
            def _():
                act()

        project_query(h, q_s)
        await_keys(h, STAY)
        attend(h, q_s, me, put_own(h))
        keep(h).start()

    lax.fori_loop(0, pairs, pair, None)

    def collect(i, _):
        @pl.when(jnp.logical_not(early))
        def _():
            result(i).wait_recv()
            keep(2 * i + MOVED).start()
            query(i).wait_send()

        @pl.when(early)
        def _():
            result(i).wait_send()

    lax.fori_loop(0, pairs, collect, None)
    go.finish()
    loads[4].wait()
    for g in (gk, gv, go, *gq):
        g.drain()

    def end(i, _):
        for sort in (MOVED, STAY):
            drain(2 * i + sort, sort)
            keep(2 * i + sort).wait()

    lax.fori_loop(0, pairs, end, None)


def solution(mesh):
    ring = mesh.shape["sp"]

    def step(x, gain, wq, wk, wv, wo):
        own, depth = x.shape
        heads = wk.shape[1] // HEAD
        half = HEAD // 2
        freq = THETA ** (-jnp.arange(half, dtype=jnp.float32) / half)
        freq = jnp.concatenate([freq, freq])[None]
        full = lambda w: pltpu.VMEM((w.shape[0] * ring, w.shape[1]), w.dtype)
        anywhere, vmem = pl.BlockSpec(memory_space=pl.ANY), pl.BlockSpec(memory_space=pltpu.VMEM)
        strips = own // STRIP
        seen, wof = pl.pallas_call(
            functools.partial(kernel, ring),
            out_shape=[jax.ShapeDtypeStruct((own, wq.shape[1]), x.dtype), jax.ShapeDtypeStruct((wo.shape[0] * ring, wo.shape[1]), wo.dtype)],
            in_specs=[anywhere, vmem, vmem, anywhere, anywhere, anywhere, anywhere],
            out_specs=[anywhere, anywhere],
            scratch_shapes=[
                pltpu.VMEM((own, depth), jnp.bfloat16),
                full(wk),
                full(wv),
                full(wq),
                pltpu.VMEM((strips, 2 * STRIP, HEAD), jnp.bfloat16),
                pltpu.VMEM((heads // 2, strips, 2 * STRIP, HEAD), jnp.bfloat16),
                pltpu.VMEM((ring, heads, 2, own, HEAD), jnp.bfloat16),
                pltpu.VMEM((heads // 2, own, 2 * HEAD), jnp.bfloat16),
                pltpu.VMEM((own, wq.shape[1]), jnp.bfloat16),
                pltpu.VMEM((own, HEAD), jnp.float32),
                pltpu.VMEM((own, HEAD), jnp.float32),
                pltpu.VMEM((strips, 2 * STRIP), jnp.float32),
                pltpu.VMEM((strips, HEAD + 8, 2 * STRIP), jnp.float32),
                pltpu.SemaphoreType.DMA((5,)),
                pltpu.SemaphoreType.DMA((heads,)),
                pltpu.SemaphoreType.DMA((3 + heads // 2, 13)),
                pltpu.SemaphoreType.DMA((3 + heads // 2, 13)),
                pltpu.SemaphoreType.DMA((3, 2, heads)),
                pltpu.SemaphoreType.DMA((ring, 2, heads)),
                *[pltpu.SemaphoreType.DMA((heads // 2,))] * 4,
            ],
            compiler_params=pltpu.CompilerParams(collective_id=0, has_side_effects=True, vmem_limit_bytes=62 * 2**20),
        )(x, gain[None], freq, wq, wk, wv, wo)
        y = jnp.dot(seen, wof, preferred_element_type=jnp.float32)
        return (x.astype(jnp.float32) + y).astype(jnp.bfloat16)

    tokens, whole = P(("dp", "sp"), None), P("sp", None)
    return jax.shard_map(
        step,
        mesh=mesh,
        in_specs=(tokens, P(None), whole, whole, whole, whole),
        out_specs=tokens,
        check_vma=False,
    )
```

```python
import functools

import jax
import jax.numpy as jnp
from jax import lax
from jax.experimental import pallas as pl
from jax.experimental.pallas import tpu as pltpu
from jax.sharding import PartitionSpec as P

HEAD = 128
THETA = 10000
NEG = -1e30
HIDDEN = 2 * NEG
LOG2E = 1.4426950408889634
MESH = pl.DeviceIdType.MESH
TILE = 256
ROWS = 512
KEYS = 512
STRIP = 256
NEAR = dict(wk=64, wv=64, wq=128, wo=128)
MOVED, STAY, SPLIT = range(3)


def _dot(a, b, ca, cb):
    return lax.dot_general(a, b, (((ca,), (cb,)), ((), ())), preferred_element_type=jnp.float32)


class Gather:
    def __init__(self, at, shard, full, sems, ids, y, column=0, columns=None):
        self.shard, self.full, self.y = shard, full, y
        self.columns = pl.ds(column, columns or shard.shape[1])
        self.send, self.recv = sems[0].at[at], sems[1].at[at]
        self.me, self.left, self.right, self.far, self.core, self.near, self.c, self.p = ids
        self.rows = shard.shape[0]
        self.half = self.rows // 2
        self.n = self.half - y
        self.q = (self.n // 2 + 15) // 16 * 16

    def ring_lane(self, p, c):
        return c * self.half + p * self.y

    def near_lane(self, p, c):
        return c * self.half + p * (self.half - self.y)

    def at(self, b, off, size):
        block = (self.left, self.right, self.far)[b]
        return self.full.at[pl.ds(pl.multiple_of(block * self.rows + off, 16), size), self.columns]

    def piece(self, k, p, c):
        if k < 4:
            off, size = ((0, self.n), (0, self.n), (0, self.q), (self.q, self.n - self.q))[k]
            return self.at(min(k, 2), self.ring_lane(p, c) + off, size)
        b, kind = (k - 4) % 3, (k - 4) // 3
        return self.at(b, self.ring_lane(p, c), self.n) if kind == 1 else self.at(b, self.near_lane(p, c), self.y)

    def copy(self, src, dst, k, to):
        return pltpu.make_async_remote_copy(src, dst, self.send.at[k], self.recv.at[k], device_id=to, device_id_type=MESH)

    def arrived(self, k, p, c):
        ref = self.piece(k, p, c)
        self.copy(ref, ref, k, {"dp": self.core}).wait_recv()

    def begin(self):
        lane = self.ring_lane(self.p, self.c)
        src = self.shard.at[pl.ds(pl.multiple_of(lane, 16), self.n), self.columns]
        dst = self.full.at[pl.ds(pl.multiple_of(self.me * self.rows + lane, 16), self.n), self.columns]
        self.copy(src, dst, 0, {"sp": self.right}).start()
        self.copy(src, dst, 1, {"sp": self.left}).start()

    def hand(self, b):
        if self.y:
            ref = self.piece(4 + b, self.p, self.c)
            self.copy(ref, ref, 4 + b, {"dp": self.near}).start()
        ref = self.piece(7 + b, self.p, self.c)
        self.copy(ref, ref, 7 + b, {"dp": self.core}).start()

    def relay(self):
        lane = self.ring_lane(self.p, self.c)
        for k, off, size, to in ((0, 0, self.q, self.right), (1, self.q, self.n - self.q, self.left)):
            self.arrived(k, self.p, self.c)
            ref = self.at(k, lane + off, size)
            self.copy(ref, ref, 2 + k, {"sp": to}).start()
            self.hand(k)

    def last(self):
        for k in (2, 3):
            self.arrived(k, self.p, self.c)
        self.hand(2)

    def cross(self):
        for b in range(3 if self.y else 0):
            self.arrived(4 + b, 1 - self.p, self.c)
            ref = self.piece(10 + b, 1 - self.p, self.c)
            self.copy(ref, ref, 10 + b, {"dp": self.core}).start()

    def finish(self):
        for b in range(3):
            self.arrived(7 + b, self.p, 1 - self.c)
            if self.y:
                self.arrived(10 + b, 1 - self.p, 1 - self.c)

    def drain(self):
        for k in range(13):
            if self.y or k not in (4, 5, 6, 10, 11, 12):
                ref = self.piece(k, self.p, self.c)
                self.copy(ref, ref, k, {"dp": self.core}).wait_send()


def kernel(ring, x_ref, gain_ref, freq_ref, wq_ref, wk_ref, wv_ref, wo_ref, seen_ref, wof_ref,
           a_s, wk_s, wv_s, wq_s, q_s, moved_s, kv_s, out_s, seen_s, cos_s, sin_s, top_s, mix_s,
           local, store, wsend, wrecv, ksend, krecv, qsend, qrecv, osend, orecv):
    me, group = lax.axis_index("sp"), lax.axis_index("dp")
    left, right, far = lax.rem(me + ring - 1, ring), lax.rem(me + 1, ring), lax.rem(me + 2, ring)
    c, p = lax.rem(group, 2), lax.rem(lax.div(group, 2), 2)
    core, near = group + 1 - 2 * c, group + 2 - 4 * p
    own, depth = x_ref.shape
    heads = kv_s.shape[1]
    wide = any(NEAR.values())

    barrier = pltpu.get_barrier_semaphore()
    peers = [{"sp": left}, {"sp": right}, {"dp": core}] + ([{"dp": near}] if wide else [])
    for peer in peers:
        pl.semaphore_signal(barrier, inc=1, device_id=peer, device_id_type=MESH)
    pl.semaphore_wait(barrier, len(peers))

    ids = me, left, right, far, core, near, c, p
    sems = wsend, wrecv
    gk = Gather(0, wk_ref, wk_s, sems, ids, NEAR["wk"])
    gv = Gather(1, wv_ref, wv_s, sems, ids, NEAR["wv"])
    pairs = heads // 2
    wide_q = wq_ref.shape[1] // pairs
    go = Gather(2, wo_ref, wof_ref, sems, ids, NEAR["wo"])
    gq = [Gather(3 + i, wq_ref, wq_s, sems, ids, NEAR["wq"], i * wide_q, wide_q) for i in range(pairs)]
    gk.begin()
    gv.begin()

    def mine(full, shard):
        return full.at[pl.ds(pl.multiple_of(me * shard.shape[0], 16), shard.shape[0]), :]

    loads = [pltpu.make_async_copy(x_ref, a_s, local.at[0]), pltpu.make_async_copy(wk_ref, mine(wk_s, wk_ref), local.at[1]),
             pltpu.make_async_copy(wv_ref, mine(wv_s, wv_ref), local.at[2]), pltpu.make_async_copy(wq_ref, mine(wq_s, wq_ref), local.at[3]),
             pltpu.make_async_copy(wo_ref, mine(wof_ref, wo_ref), local.at[4])]
    for load in loads:
        load.start()

    loads[0].wait()
    gain = gain_ref[...].astype(jnp.float32)

    def norm(i, _):
        rows = pl.ds(pl.multiple_of(i * 64, 64), 64)
        wide = a_s[rows, :].astype(jnp.float32)
        scale = lax.rsqrt(jnp.mean(wide * wide, -1, keepdims=True) + 1e-6)
        a_s[rows, :] = (wide * scale * gain).astype(jnp.bfloat16)

    lax.fori_loop(0, own // 64, norm, None)

    def angles(i, _):
        rows = pl.ds(pl.multiple_of(i * 128, 128), 128)
        place = me * own + i * 128 + lax.broadcasted_iota(jnp.int32, (128, HEAD), 0)
        angle = place.astype(jnp.float32) * freq_ref[...]
        cos_s[rows, :] = jnp.cos(angle)
        sine = jnp.sin(angle)
        sin_s[rows, :] = jnp.where(lax.broadcasted_iota(jnp.int32, (128, HEAD), 1) < HEAD // 2, -sine, sine)

    lax.fori_loop(0, own // 128, angles, None)

    def turned(t, rows):
        wide = t.astype(jnp.float32)
        return (wide * cos_s[rows, :] + pltpu.roll(wide, HEAD // 2, 1) * sin_s[rows, :]).astype(jnp.bfloat16)

    def project(w_s, n, rows):
        cols = pl.ds(pl.multiple_of(n * TILE, TILE), TILE)
        return jnp.dot(a_s[rows, :], w_s[:, cols], preferred_element_type=jnp.float32).astype(jnp.bfloat16)

    def copy(j, part, h, kind, to):
        ref = kv_s.at[j, h, part]
        return pltpu.make_async_remote_copy(ref, ref, ksend.at[kind, part, h], krecv.at[j, part, h], device_id={"sp": to}, device_id_type=MESH)

    last, both = ring - 1, (0, 1)
    stay = [(0, 0, 0, both), (0, 0, 1, both), (1, 1, 0, both), (2, 2, 0, both)]
    SENDS = [(0, 0, 0, both), (1, 1, 1, both), (2, 2, 1, both), (3, 3, 0, both)], stay, stay + [(1, 1, 1, (1,))]
    PASSED = [(1, 2, 1, both)], [(last, 0, 1, both), (2, 1, 0, both)], [(last, 0, 1, both), (2, 1, 0, (0,)), (0, 1, 1, (1,))]
    late = [(1, 0), (2, 0), (2, 1), (3, 0), (3, 1), (3, 2)]
    NEEDED = [(0, 1), (0, 2), (0, 3), (1, 0), (1, 2)], late, late

    def each(rows, act):
        for device in range(ring):
            mine = [f for f in rows if f[0] == device]
            if mine:
                @pl.when(me == device)
                def _():
                    for f in mine:
                        for part in f[3]:
                            act(f[1], part, f[2])

    def send(h, sort, devices=range(ring)):
        rows = [f for f in SENDS[sort] if f[0] in devices]
        each(rows, lambda j, part, way: copy(j, part, h, way, left if way else right).start())

    def pass_on(h, sort, devices=range(ring)):
        def act(j, part, way):
            copy(j, part, h, 2, left if way else right).wait_recv()
            copy(j, part, h, 2, left if way else right).start()

        each([f for f in PASSED[sort] if f[0] in devices], act)

    def await_keys(h, sort):
        done = [(f[0], f[1], part) for f in PASSED[sort] for part in f[3]]
        rest = [(*f, 0, tuple(part for part in both if (*f, part) not in done)) for f in NEEDED[sort]]
        each([(f[0], f[1], f[2], f[3]) for f in rest], lambda j, part, way: copy(j, part, h, 2, right).wait_recv())

    def drain(h, sort):
        each(SENDS[sort], lambda j, part, way: copy(j, part, h, way, right).wait_send())
        each(PASSED[sort], lambda j, part, way: copy(j, part, h, 2, right).wait_send())

    moves = pairs - 1
    stays = [(2 * i + 1, STAY) for i in range(moves)] + [(2 * moves, SPLIT), (2 * moves + 1, SPLIT)]

    early, partner = me < ring // 2, ring - 1 - me

    def to_partner(i, ref, dst, send_sem, recv_sem):
        return pltpu.make_async_remote_copy(ref, dst, send_sem.at[i], recv_sem.at[i], device_id={"sp": partner}, device_id_type=MESH)

    def query(i):
        return to_partner(i, moved_s.at[i], moved_s.at[i], qsend, qrecv)

    def panel(ref, h):
        return ref.at[:, pl.ds(pl.multiple_of(h * 2 * HEAD, 2 * HEAD), 2 * HEAD)]

    def result(i):
        return to_partner(i, out_s.at[i], panel(seen_s, 2 * i), osend, orecv)

    def keep(h):
        return pltpu.make_async_copy(panel(seen_s, h), panel(seen_ref, h), store.at[h])

    gk.relay()
    gv.relay()
    for g in gq:
        g.begin()
    gk.last()
    gk.cross()
    gv.last()
    gk.finish()
    loads[1].wait()

    tiles = own // ROWS

    def keys(i, _):
        n, m = lax.div(i, tiles), lax.rem(i, tiles)
        rows = pl.ds(pl.multiple_of(m * ROWS, ROWS), ROWS)
        t = project(wk_s, n, rows)
        for g in range(2):
            kv_s[me, 2 * n + g, 0, rows, :] = turned(t[:, g * HEAD : (g + 1) * HEAD], rows)

    lax.fori_loop(0, heads // 2 * tiles, keys, None)

    gv.cross()
    gq[0].relay()
    gv.finish()
    loads[2].wait()

    def values(i, _):
        n, m = lax.div(i, tiles), lax.rem(i, tiles)
        rows = pl.ds(pl.multiple_of(m * ROWS, ROWS), ROWS)
        t = project(wv_s, n, rows)
        for g in range(2):
            kv_s[me, 2 * n + g, 1, rows, :] = t[:, g * HEAD : (g + 1) * HEAD]

    lax.fori_loop(0, heads // 2 * tiles, values, None)

    gq[0].last()
    for g in gq[1:]:
        g.relay()
    send(0, MOVED)
    send(*stays[0])
    send(*stays[1], (0, 1))
    loads[3].wait()
    gq[0].cross()
    gq[0].finish()

    strips = own // STRIP

    def project_query(h, ref):
        for m in range(tiles):
            rows = pl.ds(m * ROWS, ROWS)
            t = project(wq_s, h, rows)
            for g in range(2):
                u = turned(t[:, g * HEAD : (g + 1) * HEAD], rows)
                for i in range(ROWS // STRIP):
                    ref[m * (ROWS // STRIP) + i, g * STRIP : (g + 1) * STRIP, :] = u[i * STRIP : (i + 1) * STRIP, :]

    def ask(i):
        @pl.when(jnp.logical_not(early))
        def _():
            project_query(2 * i, moved_s.at[i])
            query(i).start()

    ask(0)
    for g in gq[1:]:
        g.last()
    pass_on(0, MOVED)

    e = HEAD**-0.5 * LOG2E

    def update(q, k, v, which, masked):
        scores = [_dot(k, q[s], 1, 1) for s in which]
        weights, keeps = [], []
        for s, t in zip(which, scores):
            if s == masked:
                t = jnp.where(lax.rem(lax.broadcasted_iota(jnp.int32, t.shape, 1), STRIP) >= lax.broadcasted_iota(jnp.int32, t.shape, 0), t, HIDDEN)
            old = top_s[s : s + 1, :]
            top = jnp.maximum(old, t.max(axis=0, keepdims=True))
            top_s[s : s + 1, :] = top
            weights.append(jnp.exp2((t - top) * e).astype(jnp.bfloat16))
            keeps.append(jnp.exp2((old - top) * e))
        lhs = jnp.concatenate([v.T, jnp.ones((8, v.shape[0]), jnp.bfloat16)], axis=0)
        for s, w, keep in zip(which, weights, keeps):
            mix_s[s] = mix_s[s] * keep + _dot(lhs, w, 1, 0)

    per = own // KEYS

    def attend(h, q, chunk, put):
        top_s[...] = jnp.full_like(top_s, NEG)
        mix_s[...] = jnp.zeros_like(mix_s)

        def block(j, _):
            at = pl.ds(pl.multiple_of(lax.rem(j, per) * KEYS, KEYS), KEYS)
            ch = lax.div(j, per)
            update(q, kv_s[ch, h, 0, at, :], kv_s[ch, h, 1, at, :], range(strips), None)

        lax.fori_loop(0, chunk * per, block, None)
        for b in range(strips):
            at = pl.ds(b * STRIP, STRIP)
            update(q, kv_s[chunk, h, 0, at, :], kv_s[chunk, h, 1, at, :], range(b, strips), b)
        for s in range(strips):
            out = (mix_s[s, :HEAD, :] * (1 / mix_s[s, HEAD : HEAD + 1, :])).T.astype(jnp.bfloat16)
            for g in range(2):
                put(s, g, out[g * STRIP : (g + 1) * STRIP, :])

    def put_own(h):
        def put(s, g, out):
            place = pl.ds(pl.multiple_of(h * 2 * HEAD + g * HEAD, HEAD), HEAD)
            seen_s[s * STRIP : (s + 1) * STRIP, place] = out

        return put

    def stayed(h, following, sort):
        project_query(h, q_s)
        following()
        await_keys(h, sort)
        attend(h, q_s, me, put_own(h))
        keep(h).start()

    def pair(i, _):
        more = i + 1 < moves

        @pl.when(more)
        def _():
            send(2 * i + 2, MOVED)

        for n in range(moves):
            @pl.when(i == n)
            def _():
                send(*stays[n + 2], (0, 1))

        @pl.when(i == 0)
        def _():
            go.begin()

        @pl.when(i == moves - 1)
        def _():
            pass_on(*stays[-2], (0,))

        h = 2 * i

        @pl.when(early)
        def _():
            project_query(h, q_s)

        await_keys(h, MOVED)

        @pl.when(early)
        def _():
            query(i).wait_recv()

            def put(s, g, out):
                out_s[i, s * STRIP : (s + 1) * STRIP, g * HEAD : (g + 1) * HEAD] = out

            attend(h, moved_s.at[i], partner, put)
            result(i).start()
            attend(h, q_s, me, put_own(h))
            keep(h).start()

        h = 2 * i + 1

        @pl.when(i == 0)
        def _():
            pass_on(*stays[0])

        for n in range(1, pairs):
            @pl.when(i + 1 == n)
            def _():
                gq[n].cross()
                gq[n].finish()

        @pl.when(more)
        def _():
            ask(i + 1)
            pass_on(2 * i + 2, MOVED)

        @pl.when(i == moves - 1)
        def _():
            pass_on(*stays[-1], (0,))

        @pl.when(i == 1)
        def _():
            go.relay()

        @pl.when((i == 2) & early)
        def _():
            go.last()

        def following():
            for n in range(moves):
                @pl.when(i == n)
                def _():
                    pass_on(*stays[n + 1], (2, 3))
                    send(*stays[n + 1], (2, 3))

        stayed(h, following, STAY)

    lax.fori_loop(0, moves, pair, None)

    def rest(i, _):
        @pl.when((i == 0) & jnp.logical_not(early))
        def _():
            go.last()

        def following():
            @pl.when(i == 0)
            def _():
                pass_on(*stays[-1], (2, 3))
                send(*stays[-1], (2, 3))

        stayed(2 * moves + i, following, SPLIT)

    lax.fori_loop(0, 2, rest, None)
    go.cross()

    def collect(i, _):
        @pl.when(jnp.logical_not(early))
        def _():
            result(i).wait_recv()
            keep(2 * i).start()
            query(i).wait_send()

        @pl.when(early)
        def _():
            result(i).wait_send()

    lax.fori_loop(0, moves, collect, None)
    go.finish()
    loads[4].wait()
    for g in (gk, gv, go, *gq):
        g.drain()

    for h in range(heads):
        drain(h, dict(stays).get(h, MOVED))
        keep(h).wait()


def solution(mesh):
    ring = mesh.shape["sp"]

    def step(x, gain, wq, wk, wv, wo):
        own, depth = x.shape
        heads = wk.shape[1] // HEAD
        half = HEAD // 2
        freq = THETA ** (-jnp.arange(half, dtype=jnp.float32) / half)
        freq = jnp.concatenate([freq, freq])[None]
        full = lambda w: pltpu.VMEM((w.shape[0] * ring, w.shape[1]), w.dtype)
        anywhere, vmem = pl.BlockSpec(memory_space=pl.ANY), pl.BlockSpec(memory_space=pltpu.VMEM)
        strips = own // STRIP
        seen, wof = pl.pallas_call(
            functools.partial(kernel, ring),
            out_shape=[jax.ShapeDtypeStruct((own, wq.shape[1]), x.dtype), jax.ShapeDtypeStruct((wo.shape[0] * ring, wo.shape[1]), wo.dtype)],
            in_specs=[anywhere, vmem, vmem, anywhere, anywhere, anywhere, anywhere],
            out_specs=[anywhere, anywhere],
            scratch_shapes=[
                pltpu.VMEM((own, depth), jnp.bfloat16),
                full(wk),
                full(wv),
                full(wq),
                pltpu.VMEM((strips, 2 * STRIP, HEAD), jnp.bfloat16),
                pltpu.VMEM((heads // 2 - 1, strips, 2 * STRIP, HEAD), jnp.bfloat16),
                pltpu.VMEM((ring, heads, 2, own, HEAD), jnp.bfloat16),
                pltpu.VMEM((heads // 2 - 1, own, 2 * HEAD), jnp.bfloat16),
                pltpu.VMEM((own, wq.shape[1]), jnp.bfloat16),
                pltpu.VMEM((own, HEAD), jnp.float32),
                pltpu.VMEM((own, HEAD), jnp.float32),
                pltpu.VMEM((strips, 2 * STRIP), jnp.float32),
                pltpu.VMEM((strips, HEAD + 8, 2 * STRIP), jnp.float32),
                pltpu.SemaphoreType.DMA((5,)),
                pltpu.SemaphoreType.DMA((heads,)),
                pltpu.SemaphoreType.DMA((3 + heads // 2, 13)),
                pltpu.SemaphoreType.DMA((3 + heads // 2, 13)),
                pltpu.SemaphoreType.DMA((3, 2, heads)),
                pltpu.SemaphoreType.DMA((ring, 2, heads)),
                *[pltpu.SemaphoreType.DMA((heads // 2 - 1,))] * 4,
            ],
            compiler_params=pltpu.CompilerParams(collective_id=0, has_side_effects=True, vmem_limit_bytes=62 * 2**20),
        )(x, gain[None], freq, wq, wk, wv, wo)
        y = jnp.dot(seen, wof, preferred_element_type=jnp.float32)
        return (x.astype(jnp.float32) + y).astype(jnp.bfloat16)

    tokens, whole = P(("dp", "sp"), None), P("sp", None)
    return jax.shard_map(
        step,
        mesh=mesh,
        in_specs=(tokens, P(None), whole, whole, whole, whole),
        out_specs=tokens,
        check_vma=False,
    )
```

```python
import functools

import jax
import jax.numpy as jnp
import numpy as np
from jax import lax
from jax.experimental import pallas as pl
from jax.experimental.pallas import tpu as pltpu
from jax.sharding import PartitionSpec as P

HEAD = 128
THETA = 10000
NEG = -1e30
HIDDEN = 2 * NEG
LOG2E = 1.4426950408889634
MESH = pl.DeviceIdType.MESH
TILE = 256
ROWS = 512
KEYS = 512
STRIP = 256
NEAR = dict(wk=64, wv=64, wq=128, wo=128)
MOVED, STAY, SPLIT = range(3)


def _dot(a, b, ca, cb):
    return lax.dot_general(a, b, (((ca,), (cb,)), ((), ())), preferred_element_type=jnp.float32)


class Gather:
    def __init__(self, at, shard, full, sems, ids, y, column=0, columns=None):
        self.shard, self.full, self.y = shard, full, y
        self.columns = pl.ds(column, columns or shard.shape[1])
        self.send, self.recv = sems[0].at[at], sems[1].at[at]
        self.me, self.left, self.right, self.far, self.core, self.near, self.c, self.p = ids
        self.rows = shard.shape[0]
        self.half = self.rows // 2
        self.n = self.half - y
        self.q = (self.n // 2 + 15) // 16 * 16

    def ring_lane(self, p, c):
        return c * self.half + p * self.y

    def near_lane(self, p, c):
        return c * self.half + p * (self.half - self.y)

    def at(self, b, off, size):
        block = (self.left, self.right, self.far)[b]
        return self.full.at[pl.ds(pl.multiple_of(block * self.rows + off, 16), size), self.columns]

    def piece(self, k, p, c):
        if k < 4:
            off, size = ((0, self.n), (0, self.n), (0, self.q), (self.q, self.n - self.q))[k]
            return self.at(min(k, 2), self.ring_lane(p, c) + off, size)
        b, kind = (k - 4) % 3, (k - 4) // 3
        return self.at(b, self.ring_lane(p, c), self.n) if kind == 1 else self.at(b, self.near_lane(p, c), self.y)

    def copy(self, src, dst, k, to):
        return pltpu.make_async_remote_copy(src, dst, self.send.at[k], self.recv.at[k], device_id=to, device_id_type=MESH)

    def arrived(self, k, p, c):
        ref = self.piece(k, p, c)
        self.copy(ref, ref, k, {"dp": self.core}).wait_recv()

    def begin(self, ways=(0, 1)):
        lane = self.ring_lane(self.p, self.c)
        src = self.shard.at[pl.ds(pl.multiple_of(lane, 16), self.n), self.columns]
        dst = self.full.at[pl.ds(pl.multiple_of(self.me * self.rows + lane, 16), self.n), self.columns]
        for way in ways:
            self.copy(src, dst, way, {"sp": (self.right, self.left)[way]}).start()

    def hand(self, b):
        if self.y:
            ref = self.piece(4 + b, self.p, self.c)
            self.copy(ref, ref, 4 + b, {"dp": self.near}).start()
        ref = self.piece(7 + b, self.p, self.c)
        self.copy(ref, ref, 7 + b, {"dp": self.core}).start()

    def relay(self):
        lane = self.ring_lane(self.p, self.c)
        for k, off, size, to in ((0, 0, self.q, self.right), (1, self.q, self.n - self.q, self.left)):
            self.arrived(k, self.p, self.c)
            ref = self.at(k, lane + off, size)
            self.copy(ref, ref, 2 + k, {"sp": to}).start()
            self.hand(k)

    def last(self):
        for k in (2, 3):
            self.arrived(k, self.p, self.c)
        self.hand(2)

    def cross(self):
        for b in range(3 if self.y else 0):
            self.arrived(4 + b, 1 - self.p, self.c)
            ref = self.piece(10 + b, 1 - self.p, self.c)
            self.copy(ref, ref, 10 + b, {"dp": self.core}).start()

    def finish(self):
        for b in range(3):
            self.arrived(7 + b, self.p, 1 - self.c)
            if self.y:
                self.arrived(10 + b, 1 - self.p, 1 - self.c)

    def drain(self):
        for k in range(13):
            if self.y or k not in (4, 5, 6, 10, 11, 12):
                ref = self.piece(k, self.p, self.c)
                self.copy(ref, ref, k, {"dp": self.core}).wait_send()


def kernel(ring, x_ref, gain_ref, freq_ref, wq_ref, wk_ref, wv_ref, wo_ref, seen_ref, wof_ref,
           a_s, wk_s, wv_s, wq_s, q_s, moved_s, kv_s, out_s, seen_s, cos_s, sin_s, top_s, mix_s,
           local, store, wsend, wrecv, ksend, krecv, qsend, qrecv, osend, orecv):
    me, group = lax.axis_index("sp"), lax.axis_index("dp")
    left, right, far = lax.rem(me + ring - 1, ring), lax.rem(me + 1, ring), lax.rem(me + 2, ring)
    c, p = lax.rem(group, 2), lax.rem(lax.div(group, 2), 2)
    core, near = group + 1 - 2 * c, group + 2 - 4 * p
    own, depth = x_ref.shape
    heads = kv_s.shape[1]
    wide = any(NEAR.values())

    barrier = pltpu.get_barrier_semaphore()
    peers = [{"sp": left}, {"sp": right}, {"dp": core}] + ([{"dp": near}] if wide else [])
    for peer in peers:
        pl.semaphore_signal(barrier, inc=1, device_id=peer, device_id_type=MESH)
    pl.semaphore_wait(barrier, len(peers))

    ids = me, left, right, far, core, near, c, p
    sems = wsend, wrecv
    gk = Gather(0, wk_ref, wk_s, sems, ids, NEAR["wk"])
    gv = Gather(1, wv_ref, wv_s, sems, ids, NEAR["wv"])
    pairs = heads // 2
    wide_q = wq_ref.shape[1] // pairs
    go = Gather(2, wo_ref, wof_ref, sems, ids, NEAR["wo"])
    gq = [Gather(3 + i, wq_ref, wq_s, sems, ids, NEAR["wq"], i * wide_q, wide_q) for i in range(pairs)]
    gk.begin()
    gv.begin()

    def mine(full, shard):
        return full.at[pl.ds(pl.multiple_of(me * shard.shape[0], 16), shard.shape[0]), :]

    loads = [pltpu.make_async_copy(x_ref, a_s, local.at[0]), pltpu.make_async_copy(wk_ref, mine(wk_s, wk_ref), local.at[1]),
             pltpu.make_async_copy(wv_ref, mine(wv_s, wv_ref), local.at[2]), pltpu.make_async_copy(wq_ref, mine(wq_s, wq_ref), local.at[3]),
             pltpu.make_async_copy(wo_ref, mine(wof_ref, wo_ref), local.at[4])]
    for load in loads:
        load.start()

    loads[0].wait()
    gain = gain_ref[...].reshape(1, -1).astype(jnp.float32)

    def norm(i, _):
        rows = pl.ds(pl.multiple_of(i * 64, 64), 64)
        wide = a_s[rows, :].astype(jnp.float32)
        scale = lax.rsqrt(jnp.mean(wide * wide, -1, keepdims=True) + 1e-6)
        a_s[rows, :] = (wide * scale * gain).astype(jnp.bfloat16)

    lax.fori_loop(0, own // 64, norm, None)

    def angles(i, _):
        rows = pl.ds(pl.multiple_of(i * 128, 128), 128)
        place = me * own + i * 128 + lax.broadcasted_iota(jnp.int32, (128, HEAD), 0)
        angle = place.astype(jnp.float32) * freq_ref[...]
        cos_s[rows, :] = jnp.cos(angle)
        sine = jnp.sin(angle)
        sin_s[rows, :] = jnp.where(lax.broadcasted_iota(jnp.int32, (128, HEAD), 1) < HEAD // 2, -sine, sine)

    lax.fori_loop(0, own // 128, angles, None)

    def turned(t, rows):
        wide = t.astype(jnp.float32)
        return (wide * cos_s[rows, :] + pltpu.roll(wide, HEAD // 2, 1) * sin_s[rows, :]).astype(jnp.bfloat16)

    def project(w_s, n, rows):
        cols = pl.ds(pl.multiple_of(n * TILE, TILE), TILE)
        return jnp.dot(a_s[rows, :], w_s[:, cols], preferred_element_type=jnp.float32).astype(jnp.bfloat16)

    def copy(j, part, h, kind, to):
        ref = kv_s.at[j, h, part]
        return pltpu.make_async_remote_copy(ref, ref, ksend.at[kind, part, h], krecv.at[j, part, h], device_id={"sp": to}, device_id_type=MESH)

    last, both = ring - 1, (0, 1)
    stay = [(0, 0, 0, both), (0, 0, 1, both), (1, 1, 0, both), (2, 2, 0, both)]
    SENDS = [(0, 0, 0, both), (1, 1, 1, both), (2, 2, 1, both), (3, 3, 0, both)], stay, stay + [(1, 1, 1, (1,))]
    PASSED = [(1, 2, 1, both)], [(last, 0, 1, both), (2, 1, 0, both)], [(last, 0, 1, both), (2, 1, 0, (0,)), (0, 1, 1, (1,))]
    late = [(1, 0), (2, 0), (2, 1), (3, 0), (3, 1), (3, 2)]
    NEEDED = [(0, 1), (0, 2), (0, 3), (1, 0), (1, 2)], late, late

    def each(rows, act):
        for device in range(ring):
            mine = [f for f in rows if f[0] == device]
            if mine:
                @pl.when(me == device)
                def _():
                    for f in mine:
                        for part in f[3]:
                            act(f[1], part, f[2])

    SOON, LATER, VIA, PACED = ((0, 1), (1, 0)), ((0, 0),), ((1, 1),), ((2, 0), (3, 0))

    def send(h, sort, which=None):
        rows = [f for f in SENDS[sort] if which is None or (f[0], f[2]) in which]
        each(rows, lambda j, part, way: copy(j, part, h, way, left if way else right).start())

    def pass_on(h, sort, devices=range(ring)):
        def act(j, part, way):
            copy(j, part, h, 2, left if way else right).wait_recv()
            copy(j, part, h, 2, left if way else right).start()

        each([f for f in PASSED[sort] if f[0] in devices], act)

    def await_chunk(h, sort, chunk):
        done = [(f[0], f[1], part) for f in PASSED[sort] for part in f[3]]
        rows = [(*f, 0, tuple(part for part in both if (*f, part) not in done)) for f in NEEDED[sort] if f[1] == chunk]
        each(rows, lambda j, part, way: copy(j, part, h, 2, right).wait_recv())

    def drain(h, sort):
        each(SENDS[sort], lambda j, part, way: copy(j, part, h, way, right).wait_send())
        each(PASSED[sort], lambda j, part, way: copy(j, part, h, 2, right).wait_send())

    moves = pairs - 1
    stays = [(2 * i + 1, STAY) for i in range(moves)] + [(2 * moves, SPLIT), (2 * moves + 1, SPLIT)]

    early, partner = me < ring // 2, ring - 1 - me

    def to_partner(i, ref, dst, send_sem, recv_sem):
        return pltpu.make_async_remote_copy(ref, dst, send_sem.at[i], recv_sem.at[i], device_id={"sp": partner}, device_id_type=MESH)

    def query(i):
        return to_partner(i, moved_s.at[i], moved_s.at[i], qsend, qrecv)

    def panel(ref, h):
        return ref.at[:, pl.ds(pl.multiple_of(h * 2 * HEAD, 2 * HEAD), 2 * HEAD)]

    def result(i):
        return to_partner(i, out_s.at[i], panel(seen_s, 2 * i), osend, orecv)

    def keep(h):
        return pltpu.make_async_copy(panel(seen_s, h), panel(seen_ref, h), store.at[h])

    gk.relay()
    gv.relay()
    for g in gq:
        g.begin()
    gk.last()
    gk.cross()
    gv.last()
    gk.finish()
    loads[1].wait()

    tiles = own // ROWS

    def keys(i, _):
        n, m = lax.div(i, tiles), lax.rem(i, tiles)
        rows = pl.ds(pl.multiple_of(m * ROWS, ROWS), ROWS)
        t = project(wk_s, n, rows)
        for g in range(2):
            kv_s[me, 2 * n + g, 0, rows, :] = turned(t[:, g * HEAD : (g + 1) * HEAD], rows)

    lax.fori_loop(0, heads // 2 * tiles, keys, None)

    gv.cross()
    gq[0].relay()
    gv.finish()
    loads[2].wait()

    def values(i, _):
        n, m = lax.div(i, tiles), lax.rem(i, tiles)
        rows = pl.ds(pl.multiple_of(m * ROWS, ROWS), ROWS)
        t = project(wv_s, n, rows)
        for g in range(2):
            kv_s[me, 2 * n + g, 1, rows, :] = t[:, g * HEAD : (g + 1) * HEAD]

    lax.fori_loop(0, heads // 2 * tiles, values, None)

    gq[0].last()
    for g in gq[1:]:
        g.relay()
    send(0, MOVED)
    send(*stays[0])
    send(*stays[1], SOON)
    loads[3].wait()
    gq[0].cross()
    gq[0].finish()

    strips = own // STRIP

    def project_query(h, ref):
        for m in range(tiles):
            rows = pl.ds(m * ROWS, ROWS)
            t = project(wq_s, h, rows)
            for g in range(2):
                u = turned(t[:, g * HEAD : (g + 1) * HEAD], rows)
                for i in range(ROWS // STRIP):
                    ref[m * (ROWS // STRIP) + i, g * STRIP : (g + 1) * STRIP, :] = u[i * STRIP : (i + 1) * STRIP, :]

    def ask(i):
        @pl.when(jnp.logical_not(early))
        def _():
            project_query(2 * i, moved_s.at[i])
            query(i).start()

    ask(0)
    for g in gq[1:]:
        g.last()
    pass_on(0, MOVED)

    e = HEAD**-0.5 * LOG2E

    def update(q, k, v, which, masked):
        scores = [_dot(k, q[s], 1, 1) for s in which]
        weights, keeps = [], []
        for s, t in zip(which, scores):
            if s == masked:
                t = jnp.where(lax.rem(lax.broadcasted_iota(jnp.int32, t.shape, 1), STRIP) >= lax.broadcasted_iota(jnp.int32, t.shape, 0), t, HIDDEN)
            old = top_s[s : s + 1, :]
            top = jnp.maximum(old, t.max(axis=0, keepdims=True))
            top_s[s : s + 1, :] = top
            weights.append(jnp.exp2((t - top) * e).astype(jnp.bfloat16))
            keeps.append(jnp.exp2((old - top) * e))
        lhs = jnp.concatenate([v.T, jnp.ones((8, v.shape[0]), jnp.bfloat16)], axis=0)
        for s, w, keep in zip(which, weights, keeps):
            mix_s[s] = mix_s[s] * keep + _dot(lhs, w, 1, 0)

    per = own // KEYS

    def attend(h, q, chunk, put, sort, before):
        top_s[...] = jnp.full_like(top_s, NEG)
        mix_s[...] = jnp.zeros_like(mix_s)

        def block(j, _):
            if sort is not None:
                for n in range(last):
                    @pl.when(j == n * per)
                    def _():
                        await_chunk(h, sort, n)
            at = pl.ds(pl.multiple_of(lax.rem(j, per) * KEYS, KEYS), KEYS)
            ch = lax.div(j, per)
            update(q, kv_s[ch, h, 0, at, :], kv_s[ch, h, 1, at, :], range(strips), None)

        if before:
            lax.fori_loop(0, before * per, block, None)
            for n in range(ring):
                @pl.when(chunk == n)
                def _():
                    await_chunk(h, sort, n)
        for b in range(strips):
            at = pl.ds(b * STRIP, STRIP)
            update(q, kv_s[chunk, h, 0, at, :], kv_s[chunk, h, 1, at, :], range(b, strips), b)
        lax.fori_loop(before * per, chunk * per, block, None)
        for s in range(strips):
            out = (mix_s[s, :HEAD, :] * (1 / mix_s[s, HEAD : HEAD + 1, :])).T.astype(jnp.bfloat16)
            for g in range(2):
                put(s, g, out[g * STRIP : (g + 1) * STRIP, :])

    def put_own(h):
        def put(s, g, out):
            place = pl.ds(pl.multiple_of(h * 2 * HEAD + g * HEAD, HEAD), HEAD)
            seen_s[s * STRIP : (s + 1) * STRIP, place] = out

        return put

    def stayed(h, following, sort):
        project_query(h, q_s)
        following()
        attend(h, q_s, me, put_own(h), sort, 0)
        keep(h).start()

    def pair(i, _):
        more = i + 1 < moves

        @pl.when(more)
        def _():
            send(2 * i + 2, MOVED)

        for device in range(ring):
            @pl.when((i == 0) & (me == device))
            def _():
                go.begin(((0, 1), (0, 1), (0,), (1,))[device])

        for n, heads_now in ((0, ((1, LATER), (2, SOON), (3, SOON))), (1, ((2, LATER), (3, VIA))), (2, ((3, LATER), (4, VIA), (4, LATER)))):
            @pl.when(i == n)
            def _():
                for m, which in heads_now:
                    send(*stays[m], which)

        @pl.when(i == moves - 1)
        def _():
            pass_on(*stays[-2], (0,))

        h = 2 * i

        @pl.when(early)
        def _():
            project_query(h, q_s)

        @pl.when(early)
        def _():
            query(i).wait_recv()

            def put(s, g, out):
                out_s[i, s * STRIP : (s + 1) * STRIP, g * HEAD : (g + 1) * HEAD] = out

            attend(h, moved_s.at[i], partner, put, MOVED, 2)

            @pl.when(i == 1)
            def _():
                go.relay()
                send(*stays[4], SOON)

            result(i).start()
            attend(h, q_s, me, put_own(h), None, 0)
            keep(h).start()

        h = 2 * i + 1

        @pl.when(i == 0)
        def _():
            pass_on(*stays[0])

        for n in range(1, pairs):
            @pl.when(i + 1 == n)
            def _():
                gq[n].cross()
                gq[n].finish()

        @pl.when(more)
        def _():
            ask(i + 1)
            pass_on(2 * i + 2, MOVED)

        for device in range(ring // 2, ring):
            @pl.when((i == 0) & (me == device))
            def _():
                go.begin(((1,), (0,))[device - ring // 2])

        @pl.when(i == moves - 1)
        def _():
            pass_on(*stays[-1], (0,))

        @pl.when((i == 1) & jnp.logical_not(early))
        def _():
            go.relay()

        @pl.when((i == 2) & early)
        def _():
            go.last()

        def following():
            for n in range(moves):
                @pl.when(i == n)
                def _():
                    pass_on(*stays[n + 1], (2, 3))
                    send(*stays[n + 1], PACED)

        stayed(h, following, STAY)

    lax.fori_loop(0, moves, pair, None)

    def rest(i, _):
        @pl.when((i == 0) & jnp.logical_not(early))
        def _():
            go.last()

        def following():
            @pl.when(i == 0)
            def _():
                pass_on(*stays[-1], (2, 3))
                send(*stays[-1], PACED)

        stayed(2 * moves + i, following, SPLIT)

    lax.fori_loop(0, 2, rest, None)
    go.cross()

    def collect(i, _):
        @pl.when(jnp.logical_not(early))
        def _():
            result(i).wait_recv()
            keep(2 * i).start()
            query(i).wait_send()

        @pl.when(early)
        def _():
            result(i).wait_send()

    lax.fori_loop(0, moves, collect, None)
    go.finish()
    loads[4].wait()
    for g in (gk, gv, go, *gq):
        g.drain()

    for h in range(heads):
        drain(h, dict(stays).get(h, MOVED))
        keep(h).wait()


def solution(mesh):
    ring = mesh.shape["sp"]

    def step(x, gain, wq, wk, wv, wo):
        own, depth = x.shape
        heads = wk.shape[1] // HEAD
        half = HEAD // 2
        freq = np.float32(np.tile(float(THETA) ** (-np.arange(half) / half), 2)[None])
        full = lambda w: pltpu.VMEM((w.shape[0] * ring, w.shape[1]), w.dtype)
        anywhere, vmem = pl.BlockSpec(memory_space=pl.ANY), pl.BlockSpec(memory_space=pltpu.VMEM)
        strips = own // STRIP
        seen, wof = pl.pallas_call(
            functools.partial(kernel, ring),
            out_shape=[jax.ShapeDtypeStruct((own, wq.shape[1]), x.dtype), jax.ShapeDtypeStruct((wo.shape[0] * ring, wo.shape[1]), wo.dtype)],
            in_specs=[anywhere, vmem, vmem, anywhere, anywhere, anywhere, anywhere],
            out_specs=[anywhere, anywhere],
            scratch_shapes=[
                pltpu.VMEM((own, depth), jnp.bfloat16),
                full(wk),
                full(wv),
                full(wq),
                pltpu.VMEM((strips, 2 * STRIP, HEAD), jnp.bfloat16),
                pltpu.VMEM((heads // 2 - 1, strips, 2 * STRIP, HEAD), jnp.bfloat16),
                pltpu.VMEM((ring, heads, 2, own, HEAD), jnp.bfloat16),
                pltpu.VMEM((heads // 2 - 1, own, 2 * HEAD), jnp.bfloat16),
                pltpu.VMEM((own, wq.shape[1]), jnp.bfloat16),
                pltpu.VMEM((own, HEAD), jnp.float32),
                pltpu.VMEM((own, HEAD), jnp.float32),
                pltpu.VMEM((strips, 2 * STRIP), jnp.float32),
                pltpu.VMEM((strips, HEAD + 8, 2 * STRIP), jnp.float32),
                pltpu.SemaphoreType.DMA((5,)),
                pltpu.SemaphoreType.DMA((heads,)),
                pltpu.SemaphoreType.DMA((3 + heads // 2, 13)),
                pltpu.SemaphoreType.DMA((3 + heads // 2, 13)),
                pltpu.SemaphoreType.DMA((3, 2, heads)),
                pltpu.SemaphoreType.DMA((ring, 2, heads)),
                *[pltpu.SemaphoreType.DMA((heads // 2 - 1,))] * 4,
            ],
            compiler_params=pltpu.CompilerParams(collective_id=0, has_side_effects=True, vmem_limit_bytes=62 * 2**20),
        )(x, gain, freq, wq, wk, wv, wo)
        y = jnp.dot(seen, wof, preferred_element_type=jnp.float32)
        return (x.astype(jnp.float32) + y).astype(jnp.bfloat16)

    tokens, whole = P(("dp", "sp"), None), P("sp", None)
    return jax.shard_map(
        step,
        mesh=mesh,
        in_specs=(tokens, P(None), whole, whole, whole, whole),
        out_specs=tokens,
        check_vma=False,
    )
```

```python
import functools

import jax
import jax.numpy as jnp
import numpy as np
from jax import lax
from jax.experimental import pallas as pl
from jax.experimental.pallas import tpu as pltpu
from jax.sharding import PartitionSpec as P

HEAD = 128
THETA = 10000
NEG = -1e30
HIDDEN = 2 * NEG
LOG2E = 1.4426950408889634
MESH = pl.DeviceIdType.MESH
TILE = 256
ROWS = 512
KEYS = 512
STRIP = 256
NEAR = dict(wk=96, wv=96, wq=128, wo=128)
MOVED, STAY, SPLIT = range(3)


def _dot(a, b, ca, cb):
    return lax.dot_general(a, b, (((ca,), (cb,)), ((), ())), preferred_element_type=jnp.float32)


class Gather:
    def __init__(self, at, shard, full, sems, ids, y, column=0, columns=None):
        self.shard, self.full, self.y = shard, full, y
        self.columns = pl.ds(column, columns or shard.shape[1])
        self.send, self.recv = sems[0].at[at], sems[1].at[at]
        self.me, self.left, self.right, self.far, self.core, self.near, self.c, self.p = ids
        self.rows = shard.shape[0]
        self.half = self.rows // 2
        self.n = self.half - y
        self.q = (self.n // 2 + 15) // 16 * 16

    def ring_lane(self, p, c):
        return c * self.half + p * self.y

    def near_lane(self, p, c):
        return c * self.half + p * (self.half - self.y)

    def at(self, b, off, size):
        block = (self.left, self.right, self.far)[b]
        return self.full.at[pl.ds(pl.multiple_of(block * self.rows + off, 16), size), self.columns]

    def piece(self, k, p, c):
        if k < 4:
            off, size = ((0, self.n), (0, self.n), (0, self.q), (self.q, self.n - self.q))[k]
            return self.at(min(k, 2), self.ring_lane(p, c) + off, size)
        b, kind = (k - 4) % 3, (k - 4) // 3
        return self.at(b, self.ring_lane(p, c), self.n) if kind == 1 else self.at(b, self.near_lane(p, c), self.y)

    def copy(self, src, dst, k, to):
        return pltpu.make_async_remote_copy(src, dst, self.send.at[k], self.recv.at[k], device_id=to, device_id_type=MESH)

    def arrived(self, k, p, c):
        ref = self.piece(k, p, c)
        self.copy(ref, ref, k, {"dp": self.core}).wait_recv()

    def begin(self, ways=(0, 1)):
        lane = self.ring_lane(self.p, self.c)
        src = self.shard.at[pl.ds(pl.multiple_of(lane, 16), self.n), self.columns]
        dst = self.full.at[pl.ds(pl.multiple_of(self.me * self.rows + lane, 16), self.n), self.columns]
        for way in ways:
            self.copy(src, dst, way, {"sp": (self.right, self.left)[way]}).start()

    def hand(self, b):
        if self.y:
            ref = self.piece(4 + b, self.p, self.c)
            self.copy(ref, ref, 4 + b, {"dp": self.near}).start()
        ref = self.piece(7 + b, self.p, self.c)
        self.copy(ref, ref, 7 + b, {"dp": self.core}).start()

    def relay(self):
        lane = self.ring_lane(self.p, self.c)
        for k, off, size, to in ((0, 0, self.q, self.right), (1, self.q, self.n - self.q, self.left)):
            self.arrived(k, self.p, self.c)
            ref = self.at(k, lane + off, size)
            self.copy(ref, ref, 2 + k, {"sp": to}).start()
            self.hand(k)

    def last(self):
        for k in (2, 3):
            self.arrived(k, self.p, self.c)
        self.hand(2)

    def cross(self):
        for b in range(3 if self.y else 0):
            self.arrived(4 + b, 1 - self.p, self.c)
            ref = self.piece(10 + b, 1 - self.p, self.c)
            self.copy(ref, ref, 10 + b, {"dp": self.core}).start()

    def finish(self):
        for b in range(3):
            self.arrived(7 + b, self.p, 1 - self.c)
            if self.y:
                self.arrived(10 + b, 1 - self.p, 1 - self.c)

    def drain(self):
        for k in range(13):
            if self.y or k not in (4, 5, 6, 10, 11, 12):
                ref = self.piece(k, self.p, self.c)
                self.copy(ref, ref, k, {"dp": self.core}).wait_send()


def kernel(ring, x_ref, gain_ref, freq_ref, wq_ref, wk_ref, wv_ref, wo_ref, seen_ref, wof_ref,
           a_s, wk_s, wv_s, wq_s, q_s, moved_s, kv_s, out_s, seen_s, cos_s, sin_s, top_s, mix_s,
           local, store, wsend, wrecv, ksend, krecv, qsend, qrecv, osend, orecv):
    me, group = lax.axis_index("sp"), lax.axis_index("dp")
    left, right, far = lax.rem(me + ring - 1, ring), lax.rem(me + 1, ring), lax.rem(me + 2, ring)
    c, p = lax.rem(group, 2), lax.rem(lax.div(group, 2), 2)
    core, near = group + 1 - 2 * c, group + 2 - 4 * p
    own, depth = x_ref.shape
    heads = kv_s.shape[1]
    wide = any(NEAR.values())

    barrier = pltpu.get_barrier_semaphore()
    peers = [{"sp": left}, {"sp": right}, {"dp": core}] + ([{"dp": near}] if wide else [])
    for peer in peers:
        pl.semaphore_signal(barrier, inc=1, device_id=peer, device_id_type=MESH)
    pl.semaphore_wait(barrier, len(peers))

    ids = me, left, right, far, core, near, c, p
    sems = wsend, wrecv
    gk = Gather(0, wk_ref, wk_s, sems, ids, NEAR["wk"])
    gv = Gather(1, wv_ref, wv_s, sems, ids, NEAR["wv"])
    pairs = heads // 2
    wide_q = wq_ref.shape[1] // pairs
    go = Gather(2, wo_ref, wof_ref, sems, ids, NEAR["wo"])
    gq = [Gather(3 + i, wq_ref, wq_s, sems, ids, NEAR["wq"], i * wide_q, wide_q) for i in range(pairs)]
    gk.begin()
    gv.begin()

    def mine(full, shard):
        return full.at[pl.ds(pl.multiple_of(me * shard.shape[0], 16), shard.shape[0]), :]

    loads = [pltpu.make_async_copy(x_ref, a_s, local.at[0]), pltpu.make_async_copy(wk_ref, mine(wk_s, wk_ref), local.at[1]),
             pltpu.make_async_copy(wv_ref, mine(wv_s, wv_ref), local.at[2]), pltpu.make_async_copy(wq_ref, mine(wq_s, wq_ref), local.at[3]),
             pltpu.make_async_copy(wo_ref, mine(wof_ref, wo_ref), local.at[4])]
    for load in loads:
        load.start()

    loads[0].wait()
    gain = gain_ref[...].reshape(1, -1).astype(jnp.float32)

    def norm(i, _):
        rows = pl.ds(pl.multiple_of(i * 64, 64), 64)
        wide = a_s[rows, :].astype(jnp.float32)
        scale = lax.rsqrt(jnp.mean(wide * wide, -1, keepdims=True) + 1e-6)
        a_s[rows, :] = (wide * scale * gain).astype(jnp.bfloat16)

    lax.fori_loop(0, own // 64, norm, None)

    def angles(i, _):
        rows = pl.ds(pl.multiple_of(i * 128, 128), 128)
        place = me * own + i * 128 + lax.broadcasted_iota(jnp.int32, (128, HEAD), 0)
        angle = place.astype(jnp.float32) * freq_ref[...]
        cos_s[rows, :] = jnp.cos(angle)
        sine = jnp.sin(angle)
        sin_s[rows, :] = jnp.where(lax.broadcasted_iota(jnp.int32, (128, HEAD), 1) < HEAD // 2, -sine, sine)

    lax.fori_loop(0, own // 128, angles, None)

    def turned(t, rows):
        wide = t.astype(jnp.float32)
        return (wide * cos_s[rows, :] + pltpu.roll(wide, HEAD // 2, 1) * sin_s[rows, :]).astype(jnp.bfloat16)

    def project(w_s, n, rows):
        cols = pl.ds(pl.multiple_of(n * TILE, TILE), TILE)
        return jnp.dot(a_s[rows, :], w_s[:, cols], preferred_element_type=jnp.float32).astype(jnp.bfloat16)

    def copy(j, part, h, kind, to):
        ref = kv_s.at[j, h, part]
        return pltpu.make_async_remote_copy(ref, ref, ksend.at[kind, part, h], krecv.at[j, part, h], device_id={"sp": to}, device_id_type=MESH)

    last, both = ring - 1, (0, 1)
    stay = [(0, 0, 0, both), (0, 0, 1, both), (1, 1, 0, both), (2, 2, 0, both)]
    SENDS = [(0, 0, 0, both), (1, 1, 1, both), (2, 2, 1, both), (3, 3, 0, both)], stay, stay + [(1, 1, 1, (1,))]
    PASSED = [(1, 2, 1, both)], [(last, 0, 1, both), (2, 1, 0, both)], [(last, 0, 1, both), (2, 1, 0, (0,)), (0, 1, 1, (1,))]
    late = [(1, 0), (2, 0), (2, 1), (3, 0), (3, 1), (3, 2)]
    NEEDED = [(0, 1), (0, 2), (0, 3), (1, 0), (1, 2)], late, late

    def each(rows, act):
        for device in range(ring):
            mine = [f for f in rows if f[0] == device]
            if mine:
                @pl.when(me == device)
                def _():
                    for f in mine:
                        for part in f[3]:
                            act(f[1], part, f[2])

    SOON, LATER, VIA, PACED = ((0, 1), (1, 0)), ((0, 0),), ((1, 1),), ((2, 0), (3, 0))

    def send(h, sort, which=None):
        rows = [f for f in SENDS[sort] if which is None or (f[0], f[2]) in which]
        each(rows, lambda j, part, way: copy(j, part, h, way, left if way else right).start())

    def pass_on(h, sort, devices=range(ring)):
        def act(j, part, way):
            copy(j, part, h, 2, left if way else right).wait_recv()
            copy(j, part, h, 2, left if way else right).start()

        each([f for f in PASSED[sort] if f[0] in devices], act)

    def await_chunk(h, sort, chunk):
        done = [(f[0], f[1], part) for f in PASSED[sort] for part in f[3]]
        rows = [(*f, 0, tuple(part for part in both if (*f, part) not in done)) for f in NEEDED[sort] if f[1] == chunk]
        each(rows, lambda j, part, way: copy(j, part, h, 2, right).wait_recv())

    def drain(h, sort):
        each(SENDS[sort], lambda j, part, way: copy(j, part, h, way, right).wait_send())
        each(PASSED[sort], lambda j, part, way: copy(j, part, h, 2, right).wait_send())

    moves = pairs - 1
    stays = [(2 * i + 1, STAY) for i in range(moves)] + [(2 * moves, SPLIT), (2 * moves + 1, SPLIT)]

    early, partner = me < ring // 2, ring - 1 - me

    def to_partner(i, ref, dst, send_sem, recv_sem):
        return pltpu.make_async_remote_copy(ref, dst, send_sem.at[i], recv_sem.at[i], device_id={"sp": partner}, device_id_type=MESH)

    def query(i):
        return to_partner(i, moved_s.at[i], moved_s.at[i], qsend, qrecv)

    def panel(ref, h):
        return ref.at[:, pl.ds(pl.multiple_of(h * 2 * HEAD, 2 * HEAD), 2 * HEAD)]

    def result(i):
        return to_partner(i, out_s.at[i], panel(seen_s, 2 * i), osend, orecv)

    def keep(h):
        return pltpu.make_async_copy(panel(seen_s, h), panel(seen_ref, h), store.at[h])

    gk.relay()
    gv.relay()
    for g in gq:
        g.begin()
    go.begin()
    gk.last()
    gk.cross()
    gv.last()
    gk.finish()
    loads[1].wait()

    tiles = own // ROWS

    def keys(i, _):
        n, m = lax.div(i, tiles), lax.rem(i, tiles)
        rows = pl.ds(pl.multiple_of(m * ROWS, ROWS), ROWS)
        t = project(wk_s, n, rows)
        for g in range(2):
            kv_s[me, 2 * n + g, 0, rows, :] = turned(t[:, g * HEAD : (g + 1) * HEAD], rows)

    lax.fori_loop(0, heads // 2 * tiles, keys, None)

    gv.cross()
    gq[0].relay()
    gv.finish()
    loads[2].wait()

    def values(i, _):
        n, m = lax.div(i, tiles), lax.rem(i, tiles)
        rows = pl.ds(pl.multiple_of(m * ROWS, ROWS), ROWS)
        t = project(wv_s, n, rows)
        for g in range(2):
            kv_s[me, 2 * n + g, 1, rows, :] = t[:, g * HEAD : (g + 1) * HEAD]

    lax.fori_loop(0, heads // 2 * tiles, values, None)

    gq[0].last()
    for g in gq[1:]:
        g.relay()
    send(0, MOVED)
    send(*stays[0])
    send(*stays[1], SOON)
    loads[3].wait()
    gq[0].cross()
    gq[0].finish()

    strips = own // STRIP

    def project_query(h, ref):
        for m in range(tiles):
            rows = pl.ds(m * ROWS, ROWS)
            t = project(wq_s, h, rows)
            for g in range(2):
                u = turned(t[:, g * HEAD : (g + 1) * HEAD], rows)
                for i in range(ROWS // STRIP):
                    ref[m * (ROWS // STRIP) + i, g * STRIP : (g + 1) * STRIP, :] = u[i * STRIP : (i + 1) * STRIP, :]

    def ask(i):
        @pl.when(jnp.logical_not(early))
        def _():
            project_query(2 * i, moved_s.at[i])
            query(i).start()

    ask(0)
    for g in gq[1:]:
        g.last()
    go.relay()
    pass_on(0, MOVED)

    e = HEAD**-0.5 * LOG2E

    def update(q, k, v, which, masked):
        scores = [_dot(k, q[s], 1, 1) for s in which]
        weights, keeps = [], []
        for s, t in zip(which, scores):
            if s == masked:
                t = jnp.where(lax.rem(lax.broadcasted_iota(jnp.int32, t.shape, 1), STRIP) >= lax.broadcasted_iota(jnp.int32, t.shape, 0), t, HIDDEN)
            old = top_s[s : s + 1, :]
            top = jnp.maximum(old, t.max(axis=0, keepdims=True))
            top_s[s : s + 1, :] = top
            weights.append(jnp.exp2((t - top) * e).astype(jnp.bfloat16))
            keeps.append(jnp.exp2((old - top) * e))
        lhs = jnp.concatenate([v.T, jnp.ones((8, v.shape[0]), jnp.bfloat16)], axis=0)
        for s, w, keep in zip(which, weights, keeps):
            mix_s[s] = mix_s[s] * keep + _dot(lhs, w, 1, 0)

    per = own // KEYS

    def attend(h, q, chunk, put, sort, before):
        top_s[...] = jnp.full_like(top_s, NEG)
        mix_s[...] = jnp.zeros_like(mix_s)

        def block(j, _):
            if sort is not None:
                for n in range(last):
                    @pl.when(j == n * per)
                    def _():
                        await_chunk(h, sort, n)
            at = pl.ds(pl.multiple_of(lax.rem(j, per) * KEYS, KEYS), KEYS)
            ch = lax.div(j, per)
            update(q, kv_s[ch, h, 0, at, :], kv_s[ch, h, 1, at, :], range(strips), None)

        if before:
            lax.fori_loop(0, before * per, block, None)
            for n in range(ring):
                @pl.when(chunk == n)
                def _():
                    await_chunk(h, sort, n)
        for b in range(strips):
            at = pl.ds(b * STRIP, STRIP)
            update(q, kv_s[chunk, h, 0, at, :], kv_s[chunk, h, 1, at, :], range(b, strips), b)
        lax.fori_loop(before * per, chunk * per, block, None)
        for s in range(strips):
            out = (mix_s[s, :HEAD, :] * (1 / mix_s[s, HEAD : HEAD + 1, :])).T.astype(jnp.bfloat16)
            for g in range(2):
                put(s, g, out[g * STRIP : (g + 1) * STRIP, :])

    def put_own(h):
        def put(s, g, out):
            place = pl.ds(pl.multiple_of(h * 2 * HEAD + g * HEAD, HEAD), HEAD)
            seen_s[s * STRIP : (s + 1) * STRIP, place] = out

        return put

    def stayed(h, following, sort):
        project_query(h, q_s)
        following()
        attend(h, q_s, me, put_own(h), sort, 0)
        keep(h).start()

    def pair(i, _):
        more = i + 1 < moves

        @pl.when(more)
        def _():
            send(2 * i + 2, MOVED)

        for n, heads_now in ((0, ((1, LATER), (2, SOON), (3, SOON))), (1, ((2, LATER), (3, VIA))), (2, ((3, LATER), (4, VIA), (4, LATER)))):
            @pl.when(i == n)
            def _():
                for m, which in heads_now:
                    send(*stays[m], which)

        @pl.when(i == moves - 1)
        def _():
            pass_on(*stays[-2], (0,))

        h = 2 * i

        @pl.when(early)
        def _():
            project_query(h, q_s)

        @pl.when(early)
        def _():
            query(i).wait_recv()

            def put(s, g, out):
                out_s[i, s * STRIP : (s + 1) * STRIP, g * HEAD : (g + 1) * HEAD] = out

            attend(h, moved_s.at[i], partner, put, MOVED, 2)

            @pl.when(i == 1)
            def _():
                send(*stays[4], SOON)

            result(i).start()
            attend(h, q_s, me, put_own(h), None, 0)
            keep(h).start()

        h = 2 * i + 1

        @pl.when(i == 0)
        def _():
            pass_on(*stays[0])

        for n in range(1, pairs):
            @pl.when(i + 1 == n)
            def _():
                gq[n].cross()
                gq[n].finish()

        @pl.when(more)
        def _():
            ask(i + 1)
            pass_on(2 * i + 2, MOVED)

        @pl.when(i == moves - 1)
        def _():
            pass_on(*stays[-1], (0,))

        @pl.when(i == 0)
        def _():
            go.last()

        def following():
            for n in range(moves):
                @pl.when(i == n)
                def _():
                    pass_on(*stays[n + 1], (2, 3))
                    send(*stays[n + 1], PACED)

        stayed(h, following, STAY)

    lax.fori_loop(0, moves, pair, None)

    def rest(i, _):
        def following():
            @pl.when(i == 0)
            def _():
                pass_on(*stays[-1], (2, 3))
                send(*stays[-1], PACED)

        stayed(2 * moves + i, following, SPLIT)

    lax.fori_loop(0, 2, rest, None)
    go.cross()

    def collect(i, _):
        @pl.when(jnp.logical_not(early))
        def _():
            result(i).wait_recv()
            keep(2 * i).start()
            query(i).wait_send()

        @pl.when(early)
        def _():
            result(i).wait_send()

    lax.fori_loop(0, moves, collect, None)
    go.finish()
    loads[4].wait()
    for g in (gk, gv, go, *gq):
        g.drain()

    for h in range(heads):
        drain(h, dict(stays).get(h, MOVED))
        keep(h).wait()


def solution(mesh):
    ring = mesh.shape["sp"]

    def step(x, gain, wq, wk, wv, wo):
        own, depth = x.shape
        heads = wk.shape[1] // HEAD
        half = HEAD // 2
        freq = np.float32(np.tile(float(THETA) ** (-np.arange(half) / half), 2)[None])
        full = lambda w: pltpu.VMEM((w.shape[0] * ring, w.shape[1]), w.dtype)
        anywhere, vmem = pl.BlockSpec(memory_space=pl.ANY), pl.BlockSpec(memory_space=pltpu.VMEM)
        strips = own // STRIP
        seen, wof = pl.pallas_call(
            functools.partial(kernel, ring),
            out_shape=[jax.ShapeDtypeStruct((own, wq.shape[1]), x.dtype), jax.ShapeDtypeStruct((wo.shape[0] * ring, wo.shape[1]), wo.dtype)],
            in_specs=[anywhere, vmem, vmem, anywhere, anywhere, anywhere, anywhere],
            out_specs=[anywhere, anywhere],
            scratch_shapes=[
                pltpu.VMEM((own, depth), jnp.bfloat16),
                full(wk),
                full(wv),
                full(wq),
                pltpu.VMEM((strips, 2 * STRIP, HEAD), jnp.bfloat16),
                pltpu.VMEM((heads // 2 - 1, strips, 2 * STRIP, HEAD), jnp.bfloat16),
                pltpu.VMEM((ring, heads, 2, own, HEAD), jnp.bfloat16),
                pltpu.VMEM((heads // 2 - 1, own, 2 * HEAD), jnp.bfloat16),
                pltpu.VMEM((own, wq.shape[1]), jnp.bfloat16),
                pltpu.VMEM((own, HEAD), jnp.float32),
                pltpu.VMEM((own, HEAD), jnp.float32),
                pltpu.VMEM((strips, 2 * STRIP), jnp.float32),
                pltpu.VMEM((strips, HEAD + 8, 2 * STRIP), jnp.float32),
                pltpu.SemaphoreType.DMA((5,)),
                pltpu.SemaphoreType.DMA((heads,)),
                pltpu.SemaphoreType.DMA((3 + heads // 2, 13)),
                pltpu.SemaphoreType.DMA((3 + heads // 2, 13)),
                pltpu.SemaphoreType.DMA((3, 2, heads)),
                pltpu.SemaphoreType.DMA((ring, 2, heads)),
                *[pltpu.SemaphoreType.DMA((heads // 2 - 1,))] * 4,
            ],
            compiler_params=pltpu.CompilerParams(collective_id=0, has_side_effects=True, vmem_limit_bytes=62 * 2**20),
        )(x, gain, freq, wq, wk, wv, wo)
        y = jnp.dot(seen, wof, preferred_element_type=jnp.float32)
        return (x.astype(jnp.float32) + y).astype(jnp.bfloat16)

    tokens, whole = P(("dp", "sp"), None), P("sp", None)
    return jax.shard_map(
        step,
        mesh=mesh,
        in_specs=(tokens, P(None), whole, whole, whole, whole),
        out_specs=tokens,
        check_vma=False,
    )
```

```python
import functools

import jax
import jax.numpy as jnp
import numpy as np
from jax import lax
from jax.experimental import pallas as pl
from jax.experimental.pallas import tpu as pltpu
from jax.sharding import PartitionSpec as P

HEAD = 128
THETA = 10000
NEG = -1e30
HIDDEN = 2 * NEG
LOG2E = 1.4426950408889634
MESH = pl.DeviceIdType.MESH
TILE = 256
ROWS = 512
KEYS = 1024
DIAGONAL = 256
STRIP = 256
NEAR = dict(wk=96, wv=96, wq=128, wo=128)
MOVED, STAY, SPLIT = range(3)


def _dot(a, b, ca, cb):
    return lax.dot_general(a, b, (((ca,), (cb,)), ((), ())), preferred_element_type=jnp.float32)


class Gather:
    def __init__(self, at, shard, full, sems, ids, y, column=0, columns=None):
        self.shard, self.full, self.y = shard, full, y
        self.columns = pl.ds(column, columns or shard.shape[1])
        self.send, self.recv = sems[0].at[at], sems[1].at[at]
        self.me, self.left, self.right, self.far, self.core, self.near, self.c, self.p = ids
        self.rows = shard.shape[0]
        self.half = self.rows // 2
        self.n = self.half - y
        self.q = (self.n // 2 + 15) // 16 * 16

    def ring_lane(self, p, c):
        return c * self.half + p * self.y

    def near_lane(self, p, c):
        return c * self.half + p * (self.half - self.y)

    def at(self, b, off, size):
        block = (self.left, self.right, self.far)[b]
        return self.full.at[pl.ds(pl.multiple_of(block * self.rows + off, 16), size), self.columns]

    def piece(self, k, p, c):
        if k < 4:
            off, size = ((0, self.n), (0, self.n), (0, self.q), (self.q, self.n - self.q))[k]
            return self.at(min(k, 2), self.ring_lane(p, c) + off, size)
        b, kind = (k - 4) % 3, (k - 4) // 3
        return self.at(b, self.ring_lane(p, c), self.n) if kind == 1 else self.at(b, self.near_lane(p, c), self.y)

    def copy(self, src, dst, k, to):
        return pltpu.make_async_remote_copy(src, dst, self.send.at[k], self.recv.at[k], device_id=to, device_id_type=MESH)

    def arrived(self, k, p, c):
        ref = self.piece(k, p, c)
        self.copy(ref, ref, k, {"dp": self.core}).wait_recv()

    def begin(self, ways=(0, 1)):
        lane = self.ring_lane(self.p, self.c)
        src = self.shard.at[pl.ds(pl.multiple_of(lane, 16), self.n), self.columns]
        dst = self.full.at[pl.ds(pl.multiple_of(self.me * self.rows + lane, 16), self.n), self.columns]
        for way in ways:
            self.copy(src, dst, way, {"sp": (self.right, self.left)[way]}).start()

    def hand(self, b):
        if self.y:
            ref = self.piece(4 + b, self.p, self.c)
            self.copy(ref, ref, 4 + b, {"dp": self.near}).start()
        ref = self.piece(7 + b, self.p, self.c)
        self.copy(ref, ref, 7 + b, {"dp": self.core}).start()

    def relay(self):
        lane = self.ring_lane(self.p, self.c)
        for k, off, size, to in ((0, 0, self.q, self.right), (1, self.q, self.n - self.q, self.left)):
            self.arrived(k, self.p, self.c)
            ref = self.at(k, lane + off, size)
            self.copy(ref, ref, 2 + k, {"sp": to}).start()
            self.hand(k)

    def last(self):
        for k in (2, 3):
            self.arrived(k, self.p, self.c)
        self.hand(2)

    def cross(self):
        for b in range(3 if self.y else 0):
            self.arrived(4 + b, 1 - self.p, self.c)
            ref = self.piece(10 + b, 1 - self.p, self.c)
            self.copy(ref, ref, 10 + b, {"dp": self.core}).start()

    def finish(self):
        for b in range(3):
            self.arrived(7 + b, self.p, 1 - self.c)
            if self.y:
                self.arrived(10 + b, 1 - self.p, 1 - self.c)

    def drain(self):
        for k in range(13):
            if self.y or k not in (4, 5, 6, 10, 11, 12):
                ref = self.piece(k, self.p, self.c)
                self.copy(ref, ref, k, {"dp": self.core}).wait_send()


def kernel(ring, x_ref, gain_ref, freq_ref, wq_ref, wk_ref, wv_ref, wo_ref, seen_ref, wof_ref,
           a_s, wk_s, wv_s, wq_s, q_s, moved_s, kv_s, out_s, seen_s, cos_s, sin_s, top_s, mix_s,
           local, store, wsend, wrecv, ksend, krecv, qsend, qrecv, osend, orecv):
    me, group = lax.axis_index("sp"), lax.axis_index("dp")
    left, right, far = lax.rem(me + ring - 1, ring), lax.rem(me + 1, ring), lax.rem(me + 2, ring)
    c, p = lax.rem(group, 2), lax.rem(lax.div(group, 2), 2)
    core, near = group + 1 - 2 * c, group + 2 - 4 * p
    own, depth = x_ref.shape
    heads = kv_s.shape[1]
    wide = any(NEAR.values())

    barrier = pltpu.get_barrier_semaphore()
    peers = [{"sp": left}, {"sp": right}, {"dp": core}] + ([{"dp": near}] if wide else [])
    for peer in peers:
        pl.semaphore_signal(barrier, inc=1, device_id=peer, device_id_type=MESH)
    pl.semaphore_wait(barrier, len(peers))

    ids = me, left, right, far, core, near, c, p
    sems = wsend, wrecv
    gk = Gather(0, wk_ref, wk_s, sems, ids, NEAR["wk"])
    gv = Gather(1, wv_ref, wv_s, sems, ids, NEAR["wv"])
    pairs = heads // 2
    wide_q = wq_ref.shape[1] // pairs
    go = Gather(2, wo_ref, wof_ref, sems, ids, NEAR["wo"])
    gq = [Gather(3 + i, wq_ref, wq_s, sems, ids, NEAR["wq"], i * wide_q, wide_q) for i in range(pairs)]
    gk.begin()
    gv.begin()

    def mine(full, shard):
        return full.at[pl.ds(pl.multiple_of(me * shard.shape[0], 16), shard.shape[0]), :]

    loads = [pltpu.make_async_copy(x_ref, a_s, local.at[0]), pltpu.make_async_copy(wk_ref, mine(wk_s, wk_ref), local.at[1]),
             pltpu.make_async_copy(wv_ref, mine(wv_s, wv_ref), local.at[2]), pltpu.make_async_copy(wq_ref, mine(wq_s, wq_ref), local.at[3]),
             pltpu.make_async_copy(wo_ref, mine(wof_ref, wo_ref), local.at[4])]
    for load in loads:
        load.start()

    loads[0].wait()
    gain = gain_ref[...].reshape(1, -1).astype(jnp.float32)

    def norm(i, _):
        rows = pl.ds(pl.multiple_of(i * 64, 64), 64)
        wide = a_s[rows, :].astype(jnp.float32)
        scale = lax.rsqrt(jnp.mean(wide * wide, -1, keepdims=True) + 1e-6)
        a_s[rows, :] = (wide * scale * gain).astype(jnp.bfloat16)

    lax.fori_loop(0, own // 64, norm, None)

    def angles(i, _):
        rows = pl.ds(pl.multiple_of(i * 128, 128), 128)
        place = me * own + i * 128 + lax.broadcasted_iota(jnp.int32, (128, HEAD), 0)
        angle = place.astype(jnp.float32) * freq_ref[...]
        cos_s[rows, :] = jnp.cos(angle)
        sine = jnp.sin(angle)
        sin_s[rows, :] = jnp.where(lax.broadcasted_iota(jnp.int32, (128, HEAD), 1) < HEAD // 2, -sine, sine)

    lax.fori_loop(0, own // 128, angles, None)

    def turned(t, rows):
        wide = t.astype(jnp.float32)
        return (wide * cos_s[rows, :] + pltpu.roll(wide, HEAD // 2, 1) * sin_s[rows, :]).astype(jnp.bfloat16)

    def project(w_s, n, rows):
        cols = pl.ds(pl.multiple_of(n * TILE, TILE), TILE)
        return jnp.dot(a_s[rows, :], w_s[:, cols], preferred_element_type=jnp.float32).astype(jnp.bfloat16)

    def copy(j, part, h, kind, to):
        ref = kv_s.at[j, h, part]
        return pltpu.make_async_remote_copy(ref, ref, ksend.at[kind, part, h], krecv.at[j, part, h], device_id={"sp": to}, device_id_type=MESH)

    last, both = ring - 1, (0, 1)
    stay = [(0, 0, 0, both), (0, 0, 1, both), (1, 1, 0, both), (2, 2, 0, both)]
    SENDS = [(0, 0, 0, both), (1, 1, 1, both), (2, 2, 1, both), (3, 3, 0, both)], stay, stay + [(1, 1, 1, (1,))]
    PASSED = [(1, 2, 1, both)], [(last, 0, 1, both), (2, 1, 0, both)], [(last, 0, 1, both), (2, 1, 0, (0,)), (0, 1, 1, (1,))]
    late = [(1, 0), (2, 0), (2, 1), (3, 0), (3, 1), (3, 2)]
    NEEDED = [(0, 1), (0, 2), (0, 3), (1, 0), (1, 2)], late, late

    def each(rows, act):
        for device in range(ring):
            mine = [f for f in rows if f[0] == device]
            if mine:
                @pl.when(me == device)
                def _():
                    for f in mine:
                        for part in f[3]:
                            act(f[1], part, f[2])

    SOON, LATER, VIA, PACED = ((0, 1), (1, 0)), ((0, 0),), ((1, 1),), ((2, 0), (3, 0))

    def send(h, sort, which=None):
        rows = [f for f in SENDS[sort] if which is None or (f[0], f[2]) in which]
        each(rows, lambda j, part, way: copy(j, part, h, way, left if way else right).start())

    def pass_on(h, sort, devices=range(ring)):
        def act(j, part, way):
            copy(j, part, h, 2, left if way else right).wait_recv()
            copy(j, part, h, 2, left if way else right).start()

        each([f for f in PASSED[sort] if f[0] in devices], act)

    def await_chunk(h, sort, chunk):
        done = [(f[0], f[1], part) for f in PASSED[sort] for part in f[3]]
        rows = [(*f, 0, tuple(part for part in both if (*f, part) not in done)) for f in NEEDED[sort] if f[1] == chunk]
        each(rows, lambda j, part, way: copy(j, part, h, 2, right).wait_recv())

    def drain(h, sort):
        each(SENDS[sort], lambda j, part, way: copy(j, part, h, way, right).wait_send())
        each(PASSED[sort], lambda j, part, way: copy(j, part, h, 2, right).wait_send())

    moves = pairs - 1
    stays = [(2 * i + 1, STAY) for i in range(moves)] + [(2 * moves, SPLIT), (2 * moves + 1, SPLIT)]

    early, partner = me < ring // 2, ring - 1 - me

    def to_partner(i, ref, dst, send_sem, recv_sem):
        return pltpu.make_async_remote_copy(ref, dst, send_sem.at[i], recv_sem.at[i], device_id={"sp": partner}, device_id_type=MESH)

    def query(i):
        return to_partner(i, moved_s.at[i], moved_s.at[i], qsend, qrecv)

    def panel(ref, h):
        return ref.at[:, pl.ds(pl.multiple_of(h * 2 * HEAD, 2 * HEAD), 2 * HEAD)]

    def result(i):
        return to_partner(i, out_s.at[i], panel(seen_s, 2 * i), osend, orecv)

    def keep(h):
        return pltpu.make_async_copy(panel(seen_s, h), panel(seen_ref, h), store.at[h])

    gk.relay()
    gv.relay()
    for g in gq:
        g.begin()
    go.begin()
    gk.last()
    gk.cross()
    gv.last()
    gk.finish()
    loads[1].wait()

    tiles = own // ROWS

    def keys(i, _):
        n, m = lax.div(i, tiles), lax.rem(i, tiles)
        rows = pl.ds(pl.multiple_of(m * ROWS, ROWS), ROWS)
        t = project(wk_s, n, rows)
        for g in range(2):
            kv_s[me, 2 * n + g, 0, rows, :] = turned(t[:, g * HEAD : (g + 1) * HEAD], rows)

    lax.fori_loop(0, heads // 2 * tiles, keys, None)

    gv.cross()
    gq[0].relay()
    gv.finish()
    loads[2].wait()

    def values(i, _):
        n, m = lax.div(i, tiles), lax.rem(i, tiles)
        rows = pl.ds(pl.multiple_of(m * ROWS, ROWS), ROWS)
        t = project(wv_s, n, rows)
        for g in range(2):
            kv_s[me, 2 * n + g, 1, rows, :] = t[:, g * HEAD : (g + 1) * HEAD]

    lax.fori_loop(0, heads // 2 * tiles, values, None)

    gq[0].last()
    for g in gq[1:]:
        g.relay()
    send(0, MOVED)
    send(*stays[0])
    send(*stays[1], SOON)
    loads[3].wait()
    gq[0].cross()
    gq[0].finish()

    strips = own // STRIP

    def project_query(h, ref):
        for m in range(tiles):
            rows = pl.ds(m * ROWS, ROWS)
            t = project(wq_s, h, rows)
            for g in range(2):
                u = turned(t[:, g * HEAD : (g + 1) * HEAD], rows)
                for i in range(ROWS // STRIP):
                    ref[m * (ROWS // STRIP) + i, g * STRIP : (g + 1) * STRIP, :] = u[i * STRIP : (i + 1) * STRIP, :]

    def ask(i):
        @pl.when(jnp.logical_not(early))
        def _():
            project_query(2 * i, moved_s.at[i])
            query(i).start()

    ask(0)
    for g in gq[1:]:
        g.last()
    go.relay()
    pass_on(0, MOVED)

    e = HEAD**-0.5 * LOG2E

    def update(q, k, v, which, masked):
        scores = [_dot(k, q[s], 1, 1) for s in which]
        weights, keeps = [], []
        for s, t in zip(which, scores):
            if s in masked:
                gap = lax.rem(lax.broadcasted_iota(jnp.int32, t.shape, 1), STRIP) - lax.broadcasted_iota(jnp.int32, t.shape, 0)
                t = jnp.where(gap >= -masked[s], t, HIDDEN)
            old = top_s[s : s + 1, :]
            top = jnp.maximum(old, t.max(axis=0, keepdims=True))
            top_s[s : s + 1, :] = top
            weights.append(jnp.exp2((t - top) * e).astype(jnp.bfloat16))
            keeps.append(jnp.exp2((old - top) * e))
        lhs = jnp.concatenate([v.T, jnp.ones((8, v.shape[0]), jnp.bfloat16)], axis=0)
        for s, w, keep in zip(which, weights, keeps):
            mix_s[s] = mix_s[s] * keep + _dot(lhs, w, 1, 0)

    per = own // KEYS

    def attend(h, q, chunk, put, sort, before):
        top_s[...] = jnp.full_like(top_s, NEG)
        mix_s[...] = jnp.zeros_like(mix_s)

        def block(j, _):
            if sort is not None:
                for n in range(last):
                    @pl.when(j == n * per)
                    def _():
                        await_chunk(h, sort, n)
            at = pl.ds(pl.multiple_of(lax.rem(j, per) * KEYS, KEYS), KEYS)
            ch = lax.div(j, per)
            update(q, kv_s[ch, h, 0, at, :], kv_s[ch, h, 1, at, :], range(strips), {})

        if before:
            lax.fori_loop(0, before * per, block, None)
            for n in range(ring):
                @pl.when(chunk == n)
                def _():
                    await_chunk(h, sort, n)
        for b in range(own // DIAGONAL):
            at, s = pl.ds(b * DIAGONAL, DIAGONAL), b * DIAGONAL // STRIP
            cut = {s + n: n * STRIP for n in range(DIAGONAL // STRIP)}
            update(q, kv_s[chunk, h, 0, at, :], kv_s[chunk, h, 1, at, :], range(s, strips), cut)
        lax.fori_loop(before * per, chunk * per, block, None)
        for s in range(strips):
            out = (mix_s[s, :HEAD, :] * (1 / mix_s[s, HEAD : HEAD + 1, :])).T.astype(jnp.bfloat16)
            for g in range(2):
                put(s, g, out[g * STRIP : (g + 1) * STRIP, :])

    def put_own(h):
        def put(s, g, out):
            place = pl.ds(pl.multiple_of(h * 2 * HEAD + g * HEAD, HEAD), HEAD)
            seen_s[s * STRIP : (s + 1) * STRIP, place] = out

        return put

    def stayed(h, following, sort):
        project_query(h, q_s)
        following()
        attend(h, q_s, me, put_own(h), sort, 0)
        keep(h).start()

    def pair(i, _):
        more = i + 1 < moves

        @pl.when(more)
        def _():
            send(2 * i + 2, MOVED)

        for n, heads_now in ((0, ((1, LATER), (2, SOON), (3, SOON))), (1, ((2, LATER), (3, VIA))), (2, ((3, LATER), (4, VIA), (4, LATER)))):
            @pl.when(i == n)
            def _():
                for m, which in heads_now:
                    send(*stays[m], which)

        @pl.when(i == moves - 1)
        def _():
            pass_on(*stays[-2], (0,))

        h = 2 * i

        @pl.when(early)
        def _():
            project_query(h, q_s)

        @pl.when(early)
        def _():
            query(i).wait_recv()

            def put(s, g, out):
                out_s[i, s * STRIP : (s + 1) * STRIP, g * HEAD : (g + 1) * HEAD] = out

            attend(h, moved_s.at[i], partner, put, MOVED, 2)

            @pl.when(i == 1)
            def _():
                send(*stays[4], SOON)

            result(i).start()
            attend(h, q_s, me, put_own(h), None, 0)
            keep(h).start()

        h = 2 * i + 1

        @pl.when(i == 0)
        def _():
            pass_on(*stays[0])

        for n in range(1, pairs):
            @pl.when(i + 1 == n)
            def _():
                gq[n].cross()
                gq[n].finish()

        @pl.when(more)
        def _():
            ask(i + 1)
            pass_on(2 * i + 2, MOVED)

        @pl.when(i == moves - 1)
        def _():
            pass_on(*stays[-1], (0,))

        @pl.when(i == 0)
        def _():
            go.last()

        def following():
            for n in range(moves):
                @pl.when(i == n)
                def _():
                    pass_on(*stays[n + 1], (2, 3))
                    send(*stays[n + 1], PACED)

        stayed(h, following, STAY)

    lax.fori_loop(0, moves, pair, None)

    def rest(i, _):
        def following():
            @pl.when(i == 0)
            def _():
                pass_on(*stays[-1], (2, 3))
                send(*stays[-1], PACED)

        stayed(2 * moves + i, following, SPLIT)

    lax.fori_loop(0, 2, rest, None)
    go.cross()

    def collect(i, _):
        @pl.when(jnp.logical_not(early))
        def _():
            result(i).wait_recv()
            keep(2 * i).start()
            query(i).wait_send()

        @pl.when(early)
        def _():
            result(i).wait_send()

    lax.fori_loop(0, moves, collect, None)
    go.finish()
    loads[4].wait()
    for g in (gk, gv, go, *gq):
        g.drain()

    for h in range(heads):
        drain(h, dict(stays).get(h, MOVED))
        keep(h).wait()


def solution(mesh):
    ring = mesh.shape["sp"]

    def step(x, gain, wq, wk, wv, wo):
        own, depth = x.shape
        heads = wk.shape[1] // HEAD
        half = HEAD // 2
        freq = np.float32(np.tile(float(THETA) ** (-np.arange(half) / half), 2)[None])
        full = lambda w: pltpu.VMEM((w.shape[0] * ring, w.shape[1]), w.dtype)
        anywhere, vmem = pl.BlockSpec(memory_space=pl.ANY), pl.BlockSpec(memory_space=pltpu.VMEM)
        strips = own // STRIP
        seen, wof = pl.pallas_call(
            functools.partial(kernel, ring),
            out_shape=[jax.ShapeDtypeStruct((own, wq.shape[1]), x.dtype), jax.ShapeDtypeStruct((wo.shape[0] * ring, wo.shape[1]), wo.dtype)],
            in_specs=[anywhere, vmem, vmem, anywhere, anywhere, anywhere, anywhere],
            out_specs=[anywhere, anywhere],
            scratch_shapes=[
                pltpu.VMEM((own, depth), jnp.bfloat16),
                full(wk),
                full(wv),
                full(wq),
                pltpu.VMEM((strips, 2 * STRIP, HEAD), jnp.bfloat16),
                pltpu.VMEM((heads // 2 - 1, strips, 2 * STRIP, HEAD), jnp.bfloat16),
                pltpu.VMEM((ring, heads, 2, own, HEAD), jnp.bfloat16),
                pltpu.VMEM((heads // 2 - 1, own, 2 * HEAD), jnp.bfloat16),
                pltpu.VMEM((own, wq.shape[1]), jnp.bfloat16),
                pltpu.VMEM((own, HEAD), jnp.float32),
                pltpu.VMEM((own, HEAD), jnp.float32),
                pltpu.VMEM((strips, 2 * STRIP), jnp.float32),
                pltpu.VMEM((strips, HEAD + 8, 2 * STRIP), jnp.float32),
                pltpu.SemaphoreType.DMA((5,)),
                pltpu.SemaphoreType.DMA((heads,)),
                pltpu.SemaphoreType.DMA((3 + heads // 2, 13)),
                pltpu.SemaphoreType.DMA((3 + heads // 2, 13)),
                pltpu.SemaphoreType.DMA((3, 2, heads)),
                pltpu.SemaphoreType.DMA((ring, 2, heads)),
                *[pltpu.SemaphoreType.DMA((heads // 2 - 1,))] * 4,
            ],
            compiler_params=pltpu.CompilerParams(collective_id=0, has_side_effects=True, vmem_limit_bytes=62 * 2**20),
        )(x, gain, freq, wq, wk, wv, wo)
        y = jnp.dot(seen, wof, preferred_element_type=jnp.float32)
        return (x.astype(jnp.float32) + y).astype(jnp.bfloat16)

    tokens, whole = P(("dp", "sp"), None), P("sp", None)
    return jax.shard_map(
        step,
        mesh=mesh,
        in_specs=(tokens, P(None), whole, whole, whole, whole),
        out_specs=tokens,
        check_vma=False,
    )
```
